128 devices in a mesh: samp: 4 (over z), row: 4 (over x_lo, core), col: 8 (over x_hi, y).
Axes of the slice: x: 4 (x_hi: 2, x_lo: 2; x = x_hi * 2 + x_lo), y: 4, z: 4, core: 2. Of those that a mesh axis runs over, the one named last changes fastest.
Arguments:
- pair: float32 [4, 320, 320, 128], P('samp', 'row', 'col'), may hold values from -6 to 6
- cotangent: float32 [4, 320, 320, 128], P('samp', 'row', 'col'), may hold values from -6 to 6
- crop_length: int32 [4], P('samp'), may hold values from 160 to 320
- in_gain: float32 [128], replicated, may hold values from 0.5 to 1.5
- in_bias: float32 [128], replicated, may hold values from -1.5 to 1.5
- proj_weight: bfloat16 [128, 512], replicated, may hold values from -0.5 to 0.5
- gate_weight: bfloat16 [128, 128], replicated, may hold values from -0.5 to 0.5
- out_gain: float32 [128], replicated, may hold values from 0.5 to 1.5
- out_bias: float32 [128], replicated, may hold values from -1.5 to 1.5
- out_weight: bfloat16 [128, 128], replicated, may hold values from -0.5 to 0.5
Outputs:
- grad_pair: float32 [4, 320, 320, 128], P('samp', 'row', 'col')
- grad_in_gain: float32 [128], replicated
- grad_in_bias: float32 [128], replicated
- grad_proj_weight: float32 [128, 512], replicated
- grad_gate_weight: float32 [128, 128], replicated
- grad_out_gain: float32 [128], replicated
- grad_out_bias: float32 [128], replicated
- grad_out_weight: float32 [128, 128], replicated
The draws below stay inside these ranges and needn't reach their ends.
All inputs are finite; a program needn't handle non-finite values.
Results may differ from the reference program's by a relative error of at most 0.012.
Values may be sent and summed in bfloat16 or wider, within the bound.
No kernel may reach another device: no remote copies, remote signals or barrier semaphores. Data moves between devices by JAX's collectives and lax.ppermute only.
A program may use at most 128 MiB of HBM per device.

```python
import jax
import jax.numpy as jnp
from jax import lax

C = 128
CH = 128
L = 320
SAMPLES = 4


def with_ends(entries, key, smallest, largest):
    longest = entries.shape.index(max(entries.shape))
    spots = []
    for shift in (0, 1):
        where = [jax.random.randint(jax.random.fold_in(key, axis), (), 0, length) for axis, length in enumerate(entries.shape)]
        where[longest] = (where[longest] + shift) % entries.shape[longest]
        spots.append(tuple(where))
    return entries.at[spots[0]].set(smallest).at[spots[1]].set(largest)


def level_of(own_key, shape, pieces, low, top_value):
    loudness, own = 1.0, jax.random.fold_in(own_key, 6)
    for axis_at, shards_of in pieces:
        steps = jnp.exp(jax.random.uniform(jax.random.fold_in(own, axis_at), (shards_of,), jnp.float32, low / len(pieces), top_value / len(pieces)))
        loudness = loudness * jnp.repeat(steps, shape[axis_at] // shards_of).reshape([-1 if axis == axis_at else 1 for axis in range(len(shape))])
    return loudness


def bell_draw(stream_key, extent, deviation, limit, pieces=(), kind=jnp.bfloat16):
    loudness = level_of(stream_key, extent, pieces, -0.22, 0.18) if pieces else 1.0
    array = jax.random.normal(stream_key, extent, jnp.float32) * deviation * loudness
    return jnp.minimum(jnp.maximum(array, -limit), limit).astype(kind)


def setup_inputs(seed: int = 0) -> dict:
    seeds = jax.random.split(jax.random.key(seed), 11)
    return {
        "pair": bell_draw(seeds[0], (SAMPLES, L, L, C), 1.0, 6.0, ((0, 4), (1, 4), (2, 8)), jnp.float32),
        "cotangent": bell_draw(seeds[1], (SAMPLES, L, L, C), 1.0, 6.0, ((0, 4), (1, 4), (2, 8)), jnp.float32),
        "crop_length": with_ends(jax.random.randint(seeds[2], (SAMPLES,), L // 2, L + 1), jax.random.fold_in(seeds[2], 1), L // 2, L).astype(jnp.int32),
        "in_gain": jnp.clip(1.0 + 0.1 * jax.random.normal(seeds[3], (C,), jnp.float32), 0.5, 1.5),
        "in_bias": bell_draw(seeds[4], (C,), 0.3, 1.5, (), jnp.float32),
        "proj_weight": bell_draw(seeds[5], (C, 4 * CH), C ** -0.5, 0.5),
        "gate_weight": bell_draw(seeds[6], (C, C), C ** -0.5, 0.5),
        "out_gain": jnp.clip(1.0 + 0.1 * jax.random.normal(seeds[7], (CH,), jnp.float32), 0.5, 1.5),
        "out_bias": bell_draw(seeds[8], (CH,), 0.3, 1.5, (), jnp.float32),
        "out_weight": bell_draw(seeds[9], (CH, C), CH ** -0.5, 0.5),
    }


epsilon = 1e-05

def norm_stats(values):
    centre = lax.optimization_barrier(jnp.mean(values, axis=-1, keepdims=True))
    centered = values - centre
    variance = lax.optimization_barrier(jnp.mean(centered * centered, axis=-1, keepdims=True))
    inverse = lax.rsqrt(variance + epsilon)
    return (centered * inverse, inverse)

def norm_back(upstream, normal, inverse, weights):
    scaled = upstream * weights
    return inverse * (scaled - lax.optimization_barrier(jnp.mean(scaled, axis=-1, keepdims=True)) - normal * lax.optimization_barrier(jnp.mean(scaled * normal, axis=-1, keepdims=True)))

def reference(pair, cotangent, crop_length, in_gain, in_bias, proj_weight, gate_weight, out_gain, out_bias, out_weight):
    positions = jnp.arange(L, dtype=jnp.int32)
    live = (positions[None, :] < crop_length[:, None]).astype(jnp.float32)
    live_mask = (live[:, :, None] * live[:, None, :])[..., None]
    in_hat, in_scale = norm_stats(pair)
    normed = (in_hat * in_gain + in_bias).astype(jnp.bfloat16)
    flat_normed = normed.reshape(-1, C)
    projected = jnp.dot(flat_normed, proj_weight, preferred_element_type=jnp.float32).reshape(SAMPLES, L, L, 4 * CH)
    left_sig = jax.nn.sigmoid(projected[..., :CH])
    left_value = projected[..., CH:2 * CH]
    right_sig = jax.nn.sigmoid(projected[..., 2 * CH:3 * CH])
    right_value = projected[..., 3 * CH:]
    left_factor = (left_sig * left_value * live_mask).astype(jnp.bfloat16)
    right_factor = (right_sig * right_value * live_mask).astype(jnp.bfloat16)
    product = jnp.einsum('sikh,sjkh->sijh', left_factor.astype(jnp.float32), right_factor.astype(jnp.float32))
    tri_hat, tri_scale = norm_stats(product)
    tri_normed = (tri_hat * out_gain + out_bias).astype(jnp.bfloat16)
    flat_tri = tri_normed.reshape(-1, CH)
    out_value = jnp.dot(flat_tri, out_weight, preferred_element_type=jnp.float32)
    gate_value = jax.nn.sigmoid(jnp.dot(flat_normed, gate_weight, preferred_element_type=jnp.float32))
    flat_up = cotangent.reshape(-1, C)
    d_out = (flat_up * gate_value).astype(jnp.bfloat16)
    d_gate = (flat_up * out_value * gate_value * (1.0 - gate_value)).astype(jnp.bfloat16)
    g_out_weight = jnp.dot(flat_tri.T, d_out, preferred_element_type=jnp.float32)
    d_tri_normed = jnp.dot(d_out, out_weight.T, preferred_element_type=jnp.float32).reshape(SAMPLES, L, L, CH)
    g_out_gain = lax.optimization_barrier(jnp.sum(d_tri_normed * tri_hat, axis=(0, 1, 2)))
    g_out_bias = lax.optimization_barrier(jnp.sum(d_tri_normed, axis=(0, 1, 2)))
    d_product = norm_back(d_tri_normed, tri_hat, tri_scale, out_gain).astype(jnp.bfloat16)
    d_left = jnp.einsum('sijh,sjkh->sikh', d_product.astype(jnp.float32), right_factor.astype(jnp.float32))
    d_right = jnp.einsum('sijh,sikh->sjkh', d_product.astype(jnp.float32), left_factor.astype(jnp.float32))
    d_proj = jnp.concatenate([d_left * live_mask * left_value * left_sig * (1.0 - left_sig), d_left * live_mask * left_sig, d_right * live_mask * right_value * right_sig * (1.0 - right_sig), d_right * live_mask * right_sig], axis=-1).astype(jnp.bfloat16).reshape(-1, 4 * CH)
    g_proj_weight = jnp.dot(flat_normed.T, d_proj, preferred_element_type=jnp.float32)
    g_gate_weight = jnp.dot(flat_normed.T, d_gate, preferred_element_type=jnp.float32)
    d_normed = (jnp.dot(d_proj, proj_weight.T, preferred_element_type=jnp.float32) + jnp.dot(d_gate, gate_weight.T, preferred_element_type=jnp.float32)).reshape(SAMPLES, L, L, C)
    g_in_gain = lax.optimization_barrier(jnp.sum(d_normed * in_hat, axis=(0, 1, 2)))
    g_in_bias = lax.optimization_barrier(jnp.sum(d_normed, axis=(0, 1, 2)))
    grad_pair = norm_back(d_normed, in_hat, in_scale, in_gain)
    factor = 1.0 / L
    return (grad_pair, g_in_gain * factor, g_in_bias * factor, g_proj_weight * factor, g_gate_weight * factor, g_out_gain * factor, g_out_bias * factor, g_out_weight * factor)
```

```python
import functools

import jax
import jax.numpy as jnp
from jax import lax
from jax.experimental import pallas as pl
from jax.experimental.pallas import tpu as pltpu
from jax.sharding import PartitionSpec as P

epsilon = 1e-05

TALL = 80
WIDE = 40
CH = 128
ROWS = 4
COLS = 8
PEERS = ROWS * COLS
OWN = CH // PEERS
CELLS = TALL * WIDE
STEP = 8 * TALL
STEPS = CELLS // STEP
FULL = COLS * WIDE
PITCH = FULL + 8
JPITCH = ROWS * 128 + 8
f32 = jnp.float32
bf16 = jnp.bfloat16


def mm(a, b, ca, cb):
    return lax.dot_general(a, b, (((ca,), (cb,)), ((), ())), preferred_element_type=f32)


def sigmoid(x):
    return 0.5 * jnp.tanh(0.5 * x) + 0.5


def column(row):
    return jnp.broadcast_to(row, (CH, CH)).T


def wide(col):
    return jnp.concatenate([col] * (STEP // CH), axis=1)


def interleave():
    n = 2 * CH
    q = lax.broadcasted_iota(jnp.int32, (n, n), 0)
    p = lax.broadcasted_iota(jnp.int32, (n, n), 1)
    src = ((q >> 2) & 1) * CH + (q >> 3) * OWN + (q & 3)
    return jnp.where(src == p, 1.0, 0.0).astype(bf16)


def turned(ref):
    flat = ref.reshape(STEP, CH)
    rows = [flat[pl.ds(k, TALL, stride=8), :] for k in range(8)]
    return jnp.concatenate(rows, axis=0).T


def live_cells(lim_ref, g):
    lane = lax.broadcasted_iota(jnp.int32, (1, STEP), 1)
    k = jnp.zeros((1, STEP), jnp.int32)
    for m in range(1, 8):
        k = k + jnp.where(lane >= m * TALL, 1, 0)
    i = lane - k * TALL
    live = jnp.logical_and(i < lim_ref[0], k + g * 8 < lim_ref[1])
    return jnp.where(live, 1.0, 0.0).astype(f32)


def hat_of(x):
    centre = jnp.mean(x, axis=0, keepdims=True)
    centered = x - centre
    inverse = lax.rsqrt(jnp.mean(centered * centered, axis=0, keepdims=True) + epsilon)
    return centered * inverse, inverse


def lane_fold(x):
    out = x[:, :CH]
    for m in range(1, x.shape[1] // CH):
        out = out + x[:, m * CH : (m + 1) * CH]
    return out


def peers_of(s):
    return s >> 3, s & 7


def unfold(rows):
    n = rows.shape[0]
    lane = lax.broadcasted_iota(jnp.int32, (n, 128), 1)
    out = []
    for k in range(8):
        at = k * TALL
        m, off = at // 128, at % 128
        v = rows[:, m * 128 : (m + 1) * 128]
        if off + TALL > 128:
            v = jnp.where(lane >= off, v, rows[:, (m + 1) * 128 : (m + 2) * 128])
        out.append(pltpu.roll(v, 128 - off, 1) if off else v)
    return out


def fold(pieces):
    n = pieces[0].shape[0]
    lane = lax.broadcasted_iota(jnp.int32, (n, 128), 1)
    r = [pltpu.roll(p, (k * TALL) % 128, 1) if k else p for k, p in enumerate(pieces)]
    cols = []
    for m in range(STEP // 128):
        lo, hi = m * 128, (m + 1) * 128
        v = None
        for k in range(8):
            a, b = max(lo, k * TALL), min(hi, (k + 1) * TALL)
            if a >= b:
                continue
            v = r[k] if v is None else jnp.where(lane >= a - lo, r[k], v)
        cols.append(v)
    return jnp.concatenate(cols, axis=1)


def k1(lim_ref, pair_ref, cot_ref, ig_ref, ib_ref, w_ref, gw_ref, f_ref, do_ref, e_ref, wg_s, wv_s, gw_s, v_s):
    g = pl.program_id(0)

    @pl.when(g == 0)
    def _():
        perm = interleave()
        w = w_ref[...]
        gates = jnp.concatenate([w[:, :CH], w[:, 2 * CH : 3 * CH]], axis=1)
        values = jnp.concatenate([w[:, CH : 2 * CH], w[:, 3 * CH :]], axis=1)
        wg_s[...] = mm(perm, gates, 1, 1).astype(bf16)
        wv_s[...] = mm(perm, values, 1, 1).astype(bf16)
        gw_s[...] = gw_ref[...].astype(f32).T.astype(bf16)
        v_s[0] = column(ig_ref[...])
        v_s[1] = column(ib_ref[...])

    hat, _ = hat_of(turned(pair_ref))
    normed = (hat * wide(v_s[0]) + wide(v_s[1])).astype(bf16)
    live = live_cells(lim_ref, g)
    value = mm(wv_s[...], normed, 1, 0) * live
    factor = sigmoid(mm(wg_s[...], normed, 1, 0)) * value
    f_ref[...] = factor.astype(bf16).reshape(PEERS, 2 * OWN, STEP)
    gate = sigmoid(mm(gw_s[...], normed, 1, 0))
    up = turned(cot_ref) * gate
    do_ref[...] = up.astype(bf16)
    e_ref[...] = up * (1.0 - gate)


def k2(y_ref, l_ref, r_ref, z_ref, x_s, p_s):
    def spread(s, carry):
        r, c = peers_of(s)
        rows = y_ref[s].astype(f32)
        for g in range(STEPS):
            for k, v in enumerate(unfold(rows[:, g * STEP : (g + 1) * STEP])):
                x_s[r, pl.ds(c * WIDE + g * 8 + k, 2 * OWN, stride=PITCH), :] = v
        return carry

    lax.fori_loop(0, PEERS, spread, 0)
    lane = lax.broadcasted_iota(jnp.int32, (FULL, 128), 1)

    def matrix(t):
        parts = [jnp.where(lane < TALL, x_s[r, t * PITCH : t * PITCH + FULL, :], 0.0) for r in range(ROWS)]
        return jnp.concatenate(parts, axis=1)

    for h in range(OWN):
        left = matrix(h).astype(bf16)
        right = matrix(OWN + h)
        l_ref[h] = left
        r_ref[h] = right.astype(bf16)
        product = mm(right.T.astype(bf16), left, 1, 0)
        for r in range(ROWS):
            p_s[r, h * JPITCH : h * JPITCH + ROWS * 128, :] = product[:, r * 128 : (r + 1) * 128]

    def gather(s, carry):
        r, c = peers_of(s)
        first = (c >> 1) * 128 + (c & 1) * WIDE
        for g in range(STEPS):
            pieces = [p_s[r, pl.ds(first + g * 8 + k, OWN, stride=JPITCH), :] for k in range(8)]
            z_ref[s, :, g * STEP : (g + 1) * STEP] = fold(pieces).astype(bf16)
        return carry

    lax.fori_loop(0, PEERS, gather, 0)


def k3(z_ref, do_ref, e_ref, og_ref, ob_ref, ow_ref, dp_ref, dg_ref, gow_ref, gv_ref, z_s, owt_s, v_s):
    g = pl.program_id(0)

    @pl.when(g == 0)
    def _():
        owt_s[...] = ow_ref[...].astype(f32).T.astype(bf16)
        v_s[0] = column(og_ref[...])
        v_s[1] = column(ob_ref[...])
        gow_ref[...] = jnp.zeros_like(gow_ref)
        gv_ref[...] = jnp.zeros_like(gv_ref)

    for d in range(PEERS):
        z_s[d * OWN : (d + 1) * OWN, :] = z_ref[d].astype(f32)
    hat, inverse = hat_of(z_s[...])
    gain = wide(v_s[0])
    tri = (hat * gain + wide(v_s[1])).astype(bf16)
    d_out = do_ref[...]
    out_value = mm(owt_s[...], tri, 1, 0)
    dg_ref[...] = (e_ref[...] * out_value).astype(bf16)
    gow_ref[...] += mm(tri, d_out, 1, 1)
    up = mm(ow_ref[...], d_out, 1, 0)
    uh = up * hat
    gv_ref[0] += lane_fold(uh)
    gv_ref[1] += lane_fold(up)
    scaled = up * gain
    m1 = jnp.mean(scaled, axis=0, keepdims=True)
    m2 = jnp.mean(uh * gain, axis=0, keepdims=True)
    z_s[...] = inverse * (scaled - m1 - hat * m2)
    for d in range(PEERS):
        dp_ref[d] = z_s[d * OWN : (d + 1) * OWN, :].astype(bf16)


def k4(dp_ref, l_ref, r_ref, a_ref, x_s, o_s):
    zero = jnp.zeros((128 - TALL, 128), f32)
    for r in range(ROWS):
        for h in range(OWN):
            for q in range(ROWS):
                at = h * JPITCH + q * 128 + TALL
                x_s[r, at : at + 128 - TALL, :] = zero

    def spread(s, carry):
        r, c = peers_of(s)
        first = (c >> 1) * 128 + (c & 1) * WIDE
        rows = dp_ref[s].astype(f32)
        for g in range(STEPS):
            for k, v in enumerate(unfold(rows[:, g * STEP : (g + 1) * STEP])):
                x_s[r, pl.ds(first + g * 8 + k, OWN, stride=JPITCH), :] = v
        return carry

    lax.fori_loop(0, PEERS, spread, 0)
    lane = lax.broadcasted_iota(jnp.int32, (ROWS * 128, 128), 1)
    for h in range(OWN):
        parts = []
        for r in range(ROWS):
            x = x_s[r, h * JPITCH : h * JPITCH + ROWS * 128, :]
            parts.append(jnp.where(lane < TALL, x, 0.0).astype(bf16))
        dp = jnp.concatenate(parts, axis=1)
        d_left = mm(r_ref[h], dp, 1, 0)
        d_right = mm(l_ref[h], dp, 1, 1)
        for r in range(ROWS):
            o_s[r, h * PITCH : h * PITCH + FULL, :] = d_left[:, r * 128 : (r + 1) * 128]
            at = (OWN + h) * PITCH
            o_s[r, at : at + FULL, :] = d_right[:, r * 128 : (r + 1) * 128]

    def gather(s, carry):
        r, c = peers_of(s)
        for g in range(STEPS):
            pieces = [o_s[r, pl.ds(c * WIDE + g * 8 + k, 2 * OWN, stride=PITCH), :] for k in range(8)]
            a_ref[s, :, g * STEP : (g + 1) * STEP] = fold(pieces).astype(bf16)
        return carry

    lax.fori_loop(0, PEERS, gather, 0)


def k5(
    lim_ref, pair_ref, a_ref, dg_ref, ig_ref, ib_ref, w_ref, gw_ref, gow_ref, gv_ref,
    gp_ref, s_ref, wg_s, wv_s, bk_s, v_s, ag_s, av_s, aw_s, ai_s, pk_s,
):
    g = pl.program_id(0)

    @pl.when(g == 0)
    def _():
        perm = interleave()
        w = w_ref[...]
        gates = jnp.concatenate([w[:, :CH], w[:, 2 * CH : 3 * CH]], axis=1)
        values = jnp.concatenate([w[:, CH : 2 * CH], w[:, 3 * CH :]], axis=1)
        wg_s[...] = mm(perm, gates, 1, 1).astype(bf16)
        wv_s[...] = mm(perm, values, 1, 1).astype(bf16)
        bk_s[:, : 2 * CH] = mm(gates, perm, 1, 1).astype(bf16)
        bk_s[:, 2 * CH : 4 * CH] = mm(values, perm, 1, 1).astype(bf16)
        bk_s[:, 4 * CH :] = gw_ref[...]
        v_s[0] = column(ig_ref[...])
        v_s[1] = column(ib_ref[...])
        ag_s[...] = jnp.zeros_like(ag_s)
        av_s[...] = jnp.zeros_like(av_s)
        aw_s[...] = jnp.zeros_like(aw_s)
        ai_s[...] = jnp.zeros_like(ai_s)

    hat, inverse = hat_of(turned(pair_ref))
    gain = wide(v_s[0])
    normed = (hat * gain + wide(v_s[1])).astype(bf16)
    live = live_cells(lim_ref, g)
    d = a_ref[...].reshape(2 * CH, STEP).astype(f32) * live
    sig = sigmoid(mm(wg_s[...], normed, 1, 0))
    d_value = d * sig
    d_pre = (d_value * mm(wv_s[...], normed, 1, 0) * (1.0 - sig)).astype(bf16)
    d_value = d_value.astype(bf16)
    d_gate = dg_ref[...]
    ag_s[...] += mm(normed, d_pre, 1, 1)
    av_s[...] += mm(normed, d_value, 1, 1)
    aw_s[...] += mm(normed, d_gate, 1, 1)
    d_normed = mm(bk_s[...], jnp.concatenate([d_pre, d_value, d_gate], axis=0), 1, 0)
    dh = d_normed * hat
    ai_s[0] += lane_fold(dh)
    ai_s[1] += lane_fold(d_normed)
    scaled = d_normed * gain
    m1 = jnp.mean(scaled, axis=0, keepdims=True)
    m2 = jnp.mean(dh * gain, axis=0, keepdims=True)
    back = (inverse * (scaled - m1 - hat * m2)).T
    flat = gp_ref.reshape(STEP, CH)
    for k in range(8):
        flat[pl.ds(k, TALL, stride=8), :] = back[k * TALL : (k + 1) * TALL, :]

    @pl.when(g == STEPS - 1)
    def _():
        perm = interleave()
        gates = mm(ag_s[...].astype(bf16), perm, 1, 0)
        values = mm(av_s[...].astype(bf16), perm, 1, 0)
        lane = lax.broadcasted_iota(jnp.int32, (CH, CH), 1)
        sums = jnp.zeros((CH, CH), f32)
        for n, part in enumerate((ai_s[0], ai_s[1], gv_ref[0], gv_ref[1])):
            sums = jnp.where(lane == n, jnp.sum(part, axis=1, keepdims=True), sums)
        planes = (
            gates[:, :CH], values[:, :CH], gates[:, CH:], values[:, CH:], aw_s[...], gow_ref[...], sums,
        )
        for n, plane in enumerate(planes):
            pk_s[pl.ds(n, CH, stride=8), :] = plane
        pk_s[pl.ds(7, CH, stride=8), :] = jnp.zeros((CH, CH), f32)
        s_ref[...] = pk_s[...].astype(bf16).reshape(CH, 8, CH)


def k6(x_ref, o_ref):
    total = jnp.sum(x_ref[...].astype(f32), axis=0).astype(bf16)
    o_ref[...] = jnp.broadcast_to(total[None], o_ref.shape)


def k7(x_ref, gp_ref, gg_ref, gow_ref, gv_ref, s_s, *, factor):
    s_s[...] = x_ref[...].astype(f32).reshape(CH * 8, CH) * factor
    for q in range(4):
        gp_ref[:, q * CH : (q + 1) * CH] = s_s[pl.ds(q, CH, stride=8), :]
    gg_ref[...] = s_s[pl.ds(4, CH, stride=8), :]
    gow_ref[...] = s_s[pl.ds(5, CH, stride=8), :]
    gv_ref[...] = s_s[pl.ds(6, CH, stride=8), :].T[:8]


def whole(*shape):
    return pl.BlockSpec(shape, lambda g: (0,) * len(shape))


def tile():
    return pl.BlockSpec((TALL, 8, CH), lambda g: (0, g, 0))


def lanes(*shape):
    return pl.BlockSpec((*shape, STEP), lambda g: (0,) * len(shape) + (g,))


SMEM = pl.BlockSpec(memory_space=pltpu.SMEM)


def out(shape, dtype):
    return jax.ShapeDtypeStruct(shape, dtype)


def per_device(
    pair,
    cotangent,
    crop_length,
    in_gain,
    in_bias,
    proj_weight,
    gate_weight,
    out_gain,
    out_bias,
    out_weight,
):
    group = ("row", "col")
    everyone = ("samp", "row", "col")
    swap = functools.partial(lax.all_to_all, split_axis=0, concat_axis=0, tiled=True)
    limits = jnp.stack(
        [crop_length[0] - lax.axis_index("row") * TALL, crop_length[0] - lax.axis_index("col") * WIDE]
    )
    row = lambda v: v.reshape(1, CH)
    vm = lambda *s, dtype=f32: pltpu.VMEM(s, dtype)
    factors, d_out, slope = pl.pallas_call(
        k1,
        name="factors",
        grid=(STEPS,),
        in_specs=[SMEM, tile(), tile(), whole(1, CH), whole(1, CH), whole(CH, 4 * CH), whole(CH, CH)],
        out_specs=[lanes(PEERS, 2 * OWN), lanes(CH), lanes(CH)],
        out_shape=[out((PEERS, 2 * OWN, CELLS), bf16), out((CH, CELLS), bf16), out((CH, CELLS), f32)],
        scratch_shapes=[
            vm(2 * CH, CH, dtype=bf16), vm(2 * CH, CH, dtype=bf16), vm(CH, CH, dtype=bf16), vm(2, CH, CH),
        ],
    )(limits, pair[0], cotangent[0], row(in_gain), row(in_bias), proj_weight, gate_weight)
    factors = swap(factors, group)
    left, right, product = pl.pallas_call(
        k2,
        name="product",
        out_shape=[out((OWN, FULL, ROWS * 128), bf16)] * 2 + [out((PEERS, OWN, CELLS), bf16)],
        scratch_shapes=[vm(ROWS, 2 * OWN * PITCH, 128), vm(ROWS, OWN * JPITCH, 128)],
    )(factors)
    product = swap(product, group)
    d_product, d_gate, g_out_weight, g_out = pl.pallas_call(
        k3,
        name="middle",
        grid=(STEPS,),
        in_specs=[lanes(PEERS, OWN), lanes(CH), lanes(CH), whole(1, CH), whole(1, CH), whole(CH, CH)],
        out_specs=[lanes(PEERS, OWN), lanes(CH), whole(CH, CH), whole(2, CH, CH)],
        out_shape=[
            out((PEERS, OWN, CELLS), bf16), out((CH, CELLS), bf16), out((CH, CH), f32), out((2, CH, CH), f32),
        ],
        scratch_shapes=[vm(CH, STEP), vm(CH, CH, dtype=bf16), vm(2, CH, CH)],
    )(product, d_out, slope, row(out_gain), row(out_bias), out_weight)
    d_product = swap(d_product, group)
    d_factors = pl.pallas_call(
        k4,
        name="slopes",
        out_shape=out((PEERS, 2 * OWN, CELLS), bf16),
        scratch_shapes=[vm(ROWS, OWN * JPITCH, 128), vm(ROWS, 2 * OWN * PITCH, 128)],
    )(d_product, left, right)
    d_factors = swap(d_factors, group)
    grad_pair, packed = pl.pallas_call(
        k5,
        name="inputs",
        grid=(STEPS,),
        in_specs=[
            SMEM, tile(), lanes(PEERS, 2 * OWN), lanes(CH), whole(1, CH), whole(1, CH),
            whole(CH, 4 * CH), whole(CH, CH), whole(CH, CH), whole(2, CH, CH),
        ],
        out_specs=[tile(), whole(CH, 8, CH)],
        out_shape=[out((TALL, WIDE, CH), f32), out((CH, 8, CH), bf16)],
        scratch_shapes=[
            vm(2 * CH, CH, dtype=bf16), vm(2 * CH, CH, dtype=bf16), vm(CH, 5 * CH, dtype=bf16), vm(2, CH, CH),
            vm(CH, 2 * CH), vm(CH, 2 * CH), vm(CH, CH), vm(2, CH, CH), vm(CH * 8, CH),
        ],
    )(limits, pair[0], d_factors, d_gate, row(in_gain), row(in_bias), proj_weight, gate_weight,
      g_out_weight, g_out)
    parts = swap(packed, everyone)
    total = pl.pallas_call(k6, name="total", out_shape=out((CH, 8, CH), bf16))(parts)
    total = swap(total, everyone)
    g_proj_weight, g_gate_weight, g_out_weight, sums = pl.pallas_call(
        functools.partial(k7, factor=1.0 / FULL),
        name="unpack",
        out_shape=[out((CH, 4 * CH), f32), out((CH, CH), f32), out((CH, CH), f32), out((8, CH), f32)],
        scratch_shapes=[vm(CH * 8, CH)],
    )(total)
    return (
        grad_pair[None],
        sums[0],
        sums[1],
        g_proj_weight,
        g_gate_weight,
        sums[2],
        sums[3],
        g_out_weight,
    )


def solution(mesh):
    return jax.shard_map(
        per_device,
        mesh=mesh,
        in_specs=(
            P("samp", "row", "col", None),
            P("samp", "row", "col", None),
            P("samp"),
            P(),
            P(),
            P(),
            P(),
            P(),
            P(),
            P(),
        ),
        out_specs=(P("samp", "row", "col", None), P(), P(), P(), P(), P(), P(), P()),
        check_vma=False,
    )
```

```python
import functools

import jax
import jax.numpy as jnp
from jax import lax
from jax.experimental import pallas as pl
from jax.experimental.pallas import tpu as pltpu
from jax.sharding import PartitionSpec as P

epsilon = 1e-05

TALL = 80
WIDE = 40
CH = 128
ROWS = 4
COLS = 8
PEERS = ROWS * COLS
OWN = CH // PEERS
CELLS = TALL * WIDE
STEP = 8 * TALL
STEPS = CELLS // STEP
FULL = COLS * WIDE
PITCH = FULL + 8
JPITCH = ROWS * 128 + 8
f32 = jnp.float32
bf16 = jnp.bfloat16


def mm(a, b, ca, cb):
    return lax.dot_general(a, b, (((ca,), (cb,)), ((), ())), preferred_element_type=f32)


def sigmoid(x):
    return 0.5 * jnp.tanh(0.5 * x) + 0.5


def column(row):
    return jnp.broadcast_to(row, (CH, CH)).T


def wide(col):
    return jnp.concatenate([col] * (STEP // CH), axis=1)


def interleave():
    n = 2 * CH
    q = lax.broadcasted_iota(jnp.int32, (n, n), 0)
    p = lax.broadcasted_iota(jnp.int32, (n, n), 1)
    src = ((q >> 2) & 1) * CH + (q >> 3) * OWN + (q & 3)
    return jnp.where(src == p, 1.0, 0.0).astype(bf16)


def turned(ref):
    flat = ref.reshape(STEP, CH)
    rows = [flat[pl.ds(k, TALL, stride=8), :] for k in range(8)]
    return jnp.concatenate(rows, axis=0).T


def live_cells(crop_ref, g):
    lane = lax.broadcasted_iota(jnp.int32, (1, STEP), 1)
    k = jnp.zeros((1, STEP), jnp.int32)
    for m in range(1, 8):
        k = k + jnp.where(lane >= m * TALL, 1, 0)
    i = lane - k * TALL + lax.axis_index("row") * TALL
    k = k + (g * 8 + lax.axis_index("col") * WIDE)
    live = jnp.logical_and(i < crop_ref[0], k < crop_ref[0])
    return jnp.where(live, 1.0, 0.0).astype(f32)


def hat_of(x):
    centre = jnp.mean(x, axis=0, keepdims=True)
    centered = x - centre
    inverse = lax.rsqrt(jnp.mean(centered * centered, axis=0, keepdims=True) + epsilon)
    return centered * inverse, inverse


def lane_fold(x):
    out = x[:, :CH]
    for m in range(1, x.shape[1] // CH):
        out = out + x[:, m * CH : (m + 1) * CH]
    return out


def peers_of(s):
    return s >> 3, s & 7


def unfold(rows):
    n = rows.shape[0]
    lane = lax.broadcasted_iota(jnp.int32, (n, 128), 1)
    out = []
    for k in range(8):
        at = k * TALL
        m, off = at // 128, at % 128
        v = rows[:, m * 128 : (m + 1) * 128]
        if off + TALL > 128:
            v = jnp.where(lane >= off, v, rows[:, (m + 1) * 128 : (m + 2) * 128])
        out.append(pltpu.roll(v, 128 - off, 1) if off else v)
    return out


def fold(pieces):
    n = pieces[0].shape[0]
    lane = lax.broadcasted_iota(jnp.int32, (n, 128), 1)
    r = [pltpu.roll(p, (k * TALL) % 128, 1) if k else p for k, p in enumerate(pieces)]
    cols = []
    for m in range(STEP // 128):
        lo, hi = m * 128, (m + 1) * 128
        v = None
        for k in range(8):
            a, b = max(lo, k * TALL), min(hi, (k + 1) * TALL)
            if a >= b:
                continue
            v = r[k] if v is None else jnp.where(lane >= a - lo, r[k], v)
        cols.append(v)
    return jnp.concatenate(cols, axis=1)


def sides(w):
    gates = jnp.concatenate([w[:, :CH], w[:, 2 * CH : 3 * CH]], axis=1)
    values = jnp.concatenate([w[:, CH : 2 * CH], w[:, 3 * CH :]], axis=1)
    return gates, values


def gathered(gather, buf, ref, sem):
    part = PEERS // 4
    copies = []
    for q in range(4):
        lax.fori_loop(q * part, (q + 1) * part, gather, 0, unroll=8)
        if q:
            copies[-1].start()
        rows = pl.ds(q * part, part)
        copies.append(pltpu.make_async_copy(buf.at[rows], ref.at[rows], sem.at[q]))
    copies[-1].start()
    return copies


def k1(crop_ref, pair_ref, ig_ref, ib_ref, w_ref, f_ref, wg_s, wv_s, v_s):
    g = pl.program_id(0)

    @pl.when(g == 0)
    def _():
        perm = interleave()
        gates, values = sides(w_ref[...])
        wg_s[...] = mm(perm, gates, 1, 1).astype(bf16)
        wv_s[...] = mm(perm, values, 1, 1).astype(bf16)
        v_s[0] = column(ig_ref[...])
        v_s[1] = column(ib_ref[...])

    hat, _ = hat_of(turned(pair_ref))
    normed = (hat * wide(v_s[0]) + wide(v_s[1])).astype(bf16)
    value = mm(wv_s[...], normed, 1, 0) * live_cells(crop_ref, g)
    factor = sigmoid(mm(wg_s[...], normed, 1, 0)) * value
    f_ref[...] = factor.astype(bf16).reshape(PEERS, 2 * OWN, STEP)


def k1b(
    crop_ref, pair_ref, cot_ref, ig_ref, ib_ref, w_ref, gw_ref, n_ref, do_ref, e_ref, sv_ref, sg_ref,
    wg_s, wv_s, gw_s, v_s,
):
    g = pl.program_id(0)

    @pl.when(g == 0)
    def _():
        perm = interleave()
        gates, values = sides(w_ref[...])
        wg_s[...] = mm(perm, gates, 1, 1).astype(bf16)
        wv_s[...] = mm(perm, values, 1, 1).astype(bf16)
        gw_s[...] = gw_ref[...].astype(f32).T.astype(bf16)
        v_s[0] = column(ig_ref[...])
        v_s[1] = column(ib_ref[...])

    hat, _ = hat_of(turned(pair_ref))
    normed = (hat * wide(v_s[0]) + wide(v_s[1])).astype(bf16)
    n_ref[:CH, :] = normed
    n_ref[CH:, :] = jnp.ones((16, STEP), bf16)
    sig = sigmoid(mm(wg_s[...], normed, 1, 0))
    live_sig = sig * live_cells(crop_ref, g)
    sv_ref[...] = live_sig.astype(bf16)
    sg_ref[...] = (live_sig * mm(wv_s[...], normed, 1, 0) * (1.0 - sig)).astype(bf16)
    gate = sigmoid(mm(gw_s[...], normed, 1, 0))
    up = turned(cot_ref) * gate
    do_ref[...] = up.astype(bf16)
    e_ref[...] = up * (1.0 - gate)


def k2(y_ref, l_ref, r_ref, z_ref, x_s, p_s, l_s, r_s, z_s, sem, z_sem):
    def spread(s, carry):
        r, c = peers_of(s)
        rows = y_ref[s].astype(f32)
        for g in range(STEPS):
            for k, v in enumerate(unfold(rows[:, g * STEP : (g + 1) * STEP])):
                x_s[r, pl.ds(c * WIDE + g * 8 + k, 2 * OWN, stride=PITCH), :] = v
        return carry

    lax.fori_loop(0, PEERS, spread, 0, unroll=8)
    lane = lax.broadcasted_iota(jnp.int32, (FULL, 128), 1)

    def matrix(t):
        parts = [jnp.where(lane < TALL, x_s[r, t * PITCH : t * PITCH + FULL, :], 0.0) for r in range(ROWS)]
        return jnp.concatenate(parts, axis=1)

    for h in range(OWN):
        left = matrix(h).astype(bf16)
        right = matrix(OWN + h)
        l_s[h] = left
        r_s[h] = right.astype(bf16)
        product = mm(right.T.astype(bf16), left, 1, 0)
        for r in range(ROWS):
            p_s[r, h * JPITCH : h * JPITCH + ROWS * 128, :] = product[:, r * 128 : (r + 1) * 128]

    copies = [pltpu.make_async_copy(l_s, l_ref, sem.at[0]), pltpu.make_async_copy(r_s, r_ref, sem.at[1])]
    for copy in copies:
        copy.start()

    def gather(s, carry):
        r, c = peers_of(s)
        first = (c >> 1) * 128 + (c & 1) * WIDE
        for g in range(STEPS):
            pieces = [p_s[r, pl.ds(first + g * 8 + k, OWN, stride=JPITCH), :] for k in range(8)]
            z_s[s, :, g * STEP : (g + 1) * STEP] = fold(pieces).astype(bf16)
        return carry

    for copy in copies + gathered(gather, z_s, z_ref, z_sem):
        copy.wait()


def k3(z_ref, do_ref, og_ref, ow_ref, dp_ref, z_s, v_s):
    @pl.when(pl.program_id(0) == 0)
    def _():
        v_s[...] = column(og_ref[...])

    for d in range(PEERS):
        z_s[d * OWN : (d + 1) * OWN, :] = z_ref[d].astype(f32)
    hat, inverse = hat_of(z_s[...])
    scaled = mm(ow_ref[...], do_ref[...], 1, 0) * wide(v_s[...])
    m1 = jnp.mean(scaled, axis=0, keepdims=True)
    m2 = jnp.mean(scaled * hat, axis=0, keepdims=True)
    z_s[...] = inverse * (scaled - m1 - hat * m2)
    for d in range(PEERS):
        dp_ref[d] = z_s[d * OWN : (d + 1) * OWN, :].astype(bf16)


def k3b(
    z_ref, n_ref, do_ref, e_ref, og_ref, ob_ref, ow_ref, dg_ref, gow_ref, gv_ref, gg_ref,
    z_s, owt_s, v_s,
):
    @pl.when(pl.program_id(0) == 0)
    def _():
        owt_s[...] = ow_ref[...].astype(f32).T.astype(bf16)
        v_s[0] = column(og_ref[...])
        v_s[1] = column(ob_ref[...])
        gow_ref[...] = jnp.zeros_like(gow_ref)
        gv_ref[...] = jnp.zeros_like(gv_ref)
        gg_ref[...] = jnp.zeros_like(gg_ref)

    for d in range(PEERS):
        z_s[d * OWN : (d + 1) * OWN, :] = z_ref[d].astype(f32)
    hat, _ = hat_of(z_s[...])
    tri = (hat * wide(v_s[0]) + wide(v_s[1])).astype(bf16)
    d_out = do_ref[...]
    d_gate = (e_ref[...] * mm(owt_s[...], tri, 1, 0)).astype(bf16)
    dg_ref[...] = d_gate
    gow_ref[...] += mm(tri, d_out, 1, 1)
    gg_ref[...] += mm(n_ref[...], d_gate, 1, 1)
    up = mm(ow_ref[...], d_out, 1, 0)
    gv_ref[0] += lane_fold(up * hat)
    gv_ref[1] += lane_fold(up)


def k4(dp_ref, l_ref, r_ref, a_ref, x_s, o_s, a_s, sem):
    zero = jnp.zeros((128 - TALL, 128), f32)
    for r in range(ROWS):
        for h in range(OWN):
            for q in range(ROWS):
                at = h * JPITCH + q * 128 + TALL
                x_s[r, at : at + 128 - TALL, :] = zero

    def spread(s, carry):
        r, c = peers_of(s)
        first = (c >> 1) * 128 + (c & 1) * WIDE
        rows = dp_ref[s].astype(f32)
        for g in range(STEPS):
            for k, v in enumerate(unfold(rows[:, g * STEP : (g + 1) * STEP])):
                x_s[r, pl.ds(first + g * 8 + k, OWN, stride=JPITCH), :] = v
        return carry

    lax.fori_loop(0, PEERS, spread, 0, unroll=8)
    lane = lax.broadcasted_iota(jnp.int32, (ROWS * 128, 128), 1)
    for h in range(OWN):
        parts = []
        for r in range(ROWS):
            x = x_s[r, h * JPITCH : h * JPITCH + ROWS * 128, :]
            parts.append(jnp.where(lane < TALL, x, 0.0).astype(bf16))
        dp = jnp.concatenate(parts, axis=1)
        d_left = mm(r_ref[h], dp, 1, 0)
        d_right = mm(l_ref[h], dp, 1, 1)
        for r in range(ROWS):
            o_s[r, h * PITCH : h * PITCH + FULL, :] = d_left[:, r * 128 : (r + 1) * 128]
            at = (OWN + h) * PITCH
            o_s[r, at : at + FULL, :] = d_right[:, r * 128 : (r + 1) * 128]

    def gather(s, carry):
        r, c = peers_of(s)
        for g in range(STEPS):
            pieces = [o_s[r, pl.ds(c * WIDE + g * 8 + k, 2 * OWN, stride=PITCH), :] for k in range(8)]
            a_s[s, :, g * STEP : (g + 1) * STEP] = fold(pieces).astype(bf16)
        return carry

    for copy in gathered(gather, a_s, a_ref, sem):
        copy.wait()


def k5(
    a_ref, sv_ref, sg_ref, n_ref, ig_ref, ib_ref, w_ref, gw_ref, gow_ref, gv_ref, gg_ref,
    s_ref, ag_s, av_s, pk_s,
):
    g = pl.program_id(0)

    @pl.when(g == 0)
    def _():
        ag_s[...] = jnp.zeros_like(ag_s)
        av_s[...] = jnp.zeros_like(av_s)

    d = a_ref[...].reshape(2 * CH, STEP).astype(f32)
    normed = n_ref[...]
    ag_s[...] += mm(normed, (d * sg_ref[...].astype(f32)).astype(bf16), 1, 1)
    av_s[...] += mm(normed, (d * sv_ref[...].astype(f32)).astype(bf16), 1, 1)

    @pl.when(g == STEPS - 1)
    def _():
        perm = interleave()
        gates, values = sides(w_ref[...])
        weights = (mm(gates, perm, 1, 1), mm(values, perm, 1, 1), gw_ref[...].astype(f32))
        slope = jnp.zeros((CH, 1), f32)
        shift = jnp.zeros((CH, 1), f32)
        for weight, grad in zip(weights, (ag_s, av_s, gg_ref)):
            slope += jnp.sum(weight * grad[:CH, :], axis=1, keepdims=True)
            shift += jnp.sum(weight * grad[CH : CH + 1, :], axis=1, keepdims=True)
        gain, bias = column(ig_ref[...]), column(ib_ref[...])
        lane = lax.broadcasted_iota(jnp.int32, (CH, CH), 1)
        sums = jnp.where(lane == 0, (slope - bias * shift) / gain, jnp.where(lane == 1, shift, 0.0))
        for n in range(2):
            sums = jnp.where(lane == 2 + n, jnp.sum(gv_ref[n], axis=1, keepdims=True), sums)
        d_gates = mm(ag_s[:CH, :].astype(bf16), perm, 1, 0)
        d_values = mm(av_s[:CH, :].astype(bf16), perm, 1, 0)
        planes = (
            d_gates[:, :CH], d_values[:, :CH], d_gates[:, CH:], d_values[:, CH:],
            gg_ref[:CH, :], gow_ref[...], sums, jnp.zeros((CH, CH), f32),
        )
        for n, plane in enumerate(planes):
            pk_s[pl.ds(n, CH, stride=8), :] = plane
        s_ref[...] = pk_s[...].astype(bf16).reshape(CH, 8, CH)


def k5b(pair_ref, a_ref, sv_ref, sg_ref, dg_ref, ig_ref, w_ref, gw_ref, gp_ref, bk_s, v_s):
    @pl.when(pl.program_id(0) == 0)
    def _():
        perm = interleave()
        gates, values = sides(w_ref[...])
        bk_s[:, : 2 * CH] = mm(gates, perm, 1, 1).astype(bf16)
        bk_s[:, 2 * CH : 4 * CH] = mm(values, perm, 1, 1).astype(bf16)
        bk_s[:, 4 * CH :] = gw_ref[...]
        v_s[...] = column(ig_ref[...])

    hat, inverse = hat_of(turned(pair_ref))
    d = a_ref[...].reshape(2 * CH, STEP).astype(f32)
    d_gates = (d * sg_ref[...].astype(f32)).astype(bf16)
    d_values = (d * sv_ref[...].astype(f32)).astype(bf16)
    d_normed = mm(bk_s[...], jnp.concatenate([d_gates, d_values, dg_ref[...]], axis=0), 1, 0)
    scaled = d_normed * wide(v_s[...])
    m1 = jnp.mean(scaled, axis=0, keepdims=True)
    m2 = jnp.mean(scaled * hat, axis=0, keepdims=True)
    back = (inverse * (scaled - m1 - hat * m2)).T
    flat = gp_ref.reshape(STEP, CH)
    for k in range(8):
        flat[pl.ds(k, TALL, stride=8), :] = back[k * TALL : (k + 1) * TALL, :]


def k6(x_ref, o_ref):
    total = jnp.sum(x_ref[...].astype(f32), axis=0).astype(bf16)
    o_ref[...] = jnp.broadcast_to(total[None], o_ref.shape)


def k7(x_ref, gp_ref, gg_ref, gow_ref, *rest, factor):
    s_s = rest[-1]
    s_s[...] = x_ref[...].astype(f32).reshape(CH * 8, CH) * factor
    for q in range(4):
        gp_ref[:, q * CH : (q + 1) * CH] = s_s[pl.ds(q, CH, stride=8), :]
    gg_ref[...] = s_s[pl.ds(4, CH, stride=8), :]
    gow_ref[...] = s_s[pl.ds(5, CH, stride=8), :]
    sums = s_s[pl.ds(6, CH, stride=8), :].T
    for n in range(4):
        rest[n][...] = sums[n : n + 1]


def whole(*shape):
    return pl.BlockSpec(shape, lambda g: (0,) * len(shape))


def tile():
    return pl.BlockSpec((TALL, 8, CH), lambda g: (0, g, 0))


def lanes(*shape):
    return pl.BlockSpec((*shape, STEP), lambda g: (0,) * len(shape) + (g,))


SMEM = pl.BlockSpec(memory_space=pltpu.SMEM)
SMALL = pltpu.CompilerParams(vmem_limit_bytes=12 << 20)
LARGE = pltpu.CompilerParams(vmem_limit_bytes=22 << 20)
cost = pl.CostEstimate(flops=1_000_000_000, transcendentals=0, bytes_accessed=8_000_000)


def out(shape, dtype):
    return jax.ShapeDtypeStruct(shape, dtype)


def away(shape, dtype):
    return pltpu.HBM(shape, dtype)


def keep_away(*arrays):
    return [pltpu.with_memory_space_constraint(a, pltpu.HBM) for a in arrays]


def vm(*shape, dtype=f32):
    return pltpu.VMEM(shape, dtype)


def product_call(factors, name):
    return pl.pallas_call(
        k2,
        name=name,
        compiler_params=LARGE,
        out_specs=[pl.BlockSpec(memory_space=pltpu.HBM)] * 3,
        out_shape=[away((OWN, FULL, ROWS * 128), bf16)] * 2 + [away((PEERS, OWN, CELLS), bf16)],
        scratch_shapes=[
            vm(ROWS, 2 * OWN * PITCH, 128), vm(ROWS, OWN * JPITCH, 128),
            vm(OWN, FULL, ROWS * 128, dtype=bf16), vm(OWN, FULL, ROWS * 128, dtype=bf16),
            vm(PEERS, OWN, CELLS, dtype=bf16), pltpu.SemaphoreType.DMA((2,)), pltpu.SemaphoreType.DMA((4,)),
        ],
    )(factors)


def slopes_call(d_product, left, right, name):
    return pl.pallas_call(
        k4,
        name=name,
        compiler_params=LARGE,
        out_specs=pl.BlockSpec(memory_space=pltpu.HBM),
        out_shape=away((PEERS, 2 * OWN, CELLS), bf16),
        scratch_shapes=[
            vm(ROWS, OWN * JPITCH, 128), vm(ROWS, 2 * OWN * PITCH, 128),
            vm(PEERS, 2 * OWN, CELLS, dtype=bf16), pltpu.SemaphoreType.DMA((4,)),
        ],
    )(d_product, left, right)


def per_device(
    pair,
    cotangent,
    crop_length,
    in_gain,
    in_bias,
    proj_weight,
    gate_weight,
    out_gain,
    out_bias,
    out_weight,
):
    group = ("row", "col")
    everyone = ("samp", "row", "col")
    swap = functools.partial(lax.all_to_all, split_axis=0, concat_axis=0, tiled=True)
    row = lambda v: v.reshape(1, CH)
    wb = functools.partial(vm, dtype=bf16)
    pair, cotangent = pair[0], cotangent[0]
    in_gain, in_bias, out_gain, out_bias = map(row, (in_gain, in_bias, out_gain, out_bias))
    one, square, proj = whole(1, CH), whole(CH, CH), whole(CH, 4 * CH)
    both = (PEERS, 2 * OWN, CELLS)
    factors = pl.pallas_call(
        k1,
        name="factors",
        compiler_params=SMALL,
        grid=(STEPS,),
        in_specs=[SMEM, tile(), one, one, proj],
        out_specs=lanes(PEERS, 2 * OWN),
        out_shape=out(both, bf16),
        scratch_shapes=[wb(2 * CH, CH), wb(2 * CH, CH), vm(2, CH, CH)],
    )(crop_length, *keep_away(pair, in_gain, in_bias, proj_weight))
    factors = swap(factors, group)
    normed, d_out, slope, by_value, by_gate = pl.pallas_call(
        k1b,
        name="gate",
        compiler_params=SMALL,
        grid=(STEPS,),
        in_specs=[SMEM, tile(), tile(), one, one, proj, square],
        out_specs=[lanes(CH + 16), lanes(CH), lanes(CH), lanes(2 * CH), lanes(2 * CH)],
        out_shape=[
            away((CH + 16, CELLS), bf16), away((CH, CELLS), bf16), away((CH, CELLS), f32),
            away((2 * CH, CELLS), bf16), away((2 * CH, CELLS), bf16),
        ],
        scratch_shapes=[wb(2 * CH, CH), wb(2 * CH, CH), wb(CH, CH), vm(2, CH, CH)],
        cost_estimate=cost,
    )(crop_length, *keep_away(pair, cotangent, in_gain, in_bias, proj_weight, gate_weight))
    left, right, product = product_call(factors, "product")
    product = swap(product, group)
    d_product = pl.pallas_call(
        k3,
        name="middle",
        compiler_params=SMALL,
        grid=(STEPS,),
        in_specs=[lanes(PEERS, OWN), lanes(CH), one, square],
        out_specs=lanes(PEERS, OWN),
        out_shape=out((PEERS, OWN, CELLS), bf16),
        scratch_shapes=[vm(CH, STEP), vm(CH, CH)],
    )(product, *keep_away(d_out, out_gain, out_weight))
    d_product = swap(d_product, group)
    d_gate, g_out_weight, g_out, g_gate = pl.pallas_call(
        k3b,
        name="outputs",
        compiler_params=SMALL,
        grid=(STEPS,),
        in_specs=[lanes(PEERS, OWN), lanes(CH + 16), lanes(CH), lanes(CH), one, one, square],
        out_specs=[lanes(CH), square, whole(2, CH, CH), whole(CH + 16, CH)],
        out_shape=[
            away((CH, CELLS), bf16), away((CH, CH), f32), away((2, CH, CH), f32), away((CH + 16, CH), f32),
        ],
        scratch_shapes=[vm(CH, STEP), wb(CH, CH), vm(2, CH, CH)],
        cost_estimate=cost,
    )(product, *keep_away(normed, d_out, slope, out_gain, out_bias, out_weight))
    d_factors = slopes_call(d_product, left, right, "slopes")
    d_factors = swap(d_factors, group)
    packed = pl.pallas_call(
        k5,
        name="weights",
        compiler_params=SMALL,
        grid=(STEPS,),
        in_specs=[
            lanes(PEERS, 2 * OWN), lanes(2 * CH), lanes(2 * CH), lanes(CH + 16), one, one,
            proj, square, square, whole(2, CH, CH), whole(CH + 16, CH),
        ],
        out_specs=whole(CH, 8, CH),
        out_shape=out((CH, 8, CH), bf16),
        scratch_shapes=[vm(CH + 16, 2 * CH), vm(CH + 16, 2 * CH), vm(CH * 8, CH)],
    )(d_factors, *keep_away(by_value, by_gate, normed, in_gain, in_bias, proj_weight, gate_weight,
                            g_out_weight, g_out, g_gate))
    parts = swap(packed, everyone)
    grad_pair = pl.pallas_call(
        k5b,
        name="inputs",
        compiler_params=SMALL,
        grid=(STEPS,),
        in_specs=[
            tile(), lanes(PEERS, 2 * OWN), lanes(2 * CH), lanes(2 * CH), lanes(CH), one, proj, square,
        ],
        out_specs=tile(),
        out_shape=out((TALL, WIDE, CH), f32),
        scratch_shapes=[wb(CH, 5 * CH), vm(CH, CH)],
        cost_estimate=cost,
    )(*keep_away(pair), d_factors, *keep_away(by_value, by_gate, d_gate, in_gain, proj_weight, gate_weight))
    total = pl.pallas_call(k6, name="total", compiler_params=SMALL, out_shape=out((CH, 8, CH), bf16))(parts)
    total = swap(total, everyone)
    g_proj_weight, g_gate_weight, g_out_weight, *sums = pl.pallas_call(
        functools.partial(k7, factor=1.0 / FULL),
        name="unpack",
        compiler_params=SMALL,
        out_shape=[out((CH, 4 * CH), f32), out((CH, CH), f32), out((CH, CH), f32)] + [out((1, CH), f32)] * 4,
        scratch_shapes=[vm(CH * 8, CH)],
    )(total)
    sums = [s.reshape(CH) for s in sums]
    return (
        grad_pair[None],
        sums[0],
        sums[1],
        g_proj_weight,
        g_gate_weight,
        sums[2],
        sums[3],
        g_out_weight,
    )


def solution(mesh):
    return jax.shard_map(
        per_device,
        mesh=mesh,
        in_specs=(
            P("samp", "row", "col", None),
            P("samp", "row", "col", None),
            P("samp"),
            P(),
            P(),
            P(),
            P(),
            P(),
            P(),
            P(),
        ),
        out_specs=(P("samp", "row", "col", None), P(), P(), P(), P(), P(), P(), P()),
        check_vma=False,
    )
```

```python
import functools

import jax
import jax.numpy as jnp
from jax import lax
from jax.experimental import pallas as pl
from jax.experimental.pallas import tpu as pltpu
from jax.sharding import PartitionSpec as P

epsilon = 1e-05

TALL = 80
WIDE = 40
CH = 128
ROWS = 4
COLS = 8
PEERS = ROWS * COLS
OWN = CH // PEERS
CELLS = TALL * WIDE
STEP = 8 * TALL
STEPS = CELLS // STEP
FULL = COLS * WIDE
PITCH = FULL + 8
JPITCH = ROWS * 128 + 8
f32 = jnp.float32
bf16 = jnp.bfloat16


def mm(a, b, ca, cb):
    return lax.dot_general(a, b, (((ca,), (cb,)), ((), ())), preferred_element_type=f32)


def sigmoid(x):
    return 0.5 * jnp.tanh(0.5 * x) + 0.5


def column(row):
    return jnp.broadcast_to(row, (CH, CH)).T


def wide(col):
    return jnp.concatenate([col] * (STEP // CH), axis=1)


def interleave():
    n = 2 * CH
    q = lax.broadcasted_iota(jnp.int32, (n, n), 0)
    p = lax.broadcasted_iota(jnp.int32, (n, n), 1)
    src = ((q >> 2) & 1) * CH + (q >> 3) * OWN + (q & 3)
    return jnp.where(src == p, 1.0, 0.0).astype(bf16)


def turned(ref):
    flat = ref.reshape(STEP, CH)
    rows = [flat[pl.ds(k, TALL, stride=8), :] for k in range(8)]
    return jnp.concatenate(rows, axis=0).T


def live_cells(crop_ref, g):
    lane = lax.broadcasted_iota(jnp.int32, (1, STEP), 1)
    k = jnp.zeros((1, STEP), jnp.int32)
    for m in range(1, 8):
        k = k + jnp.where(lane >= m * TALL, 1, 0)
    i = lane - k * TALL + lax.axis_index("row") * TALL
    k = k + (g * 8 + lax.axis_index("col") * WIDE)
    live = jnp.logical_and(i < crop_ref[0], k < crop_ref[0])
    return jnp.where(live, 1.0, 0.0).astype(f32)


def hat_of(x):
    centre = jnp.mean(x, axis=0, keepdims=True)
    centered = x - centre
    inverse = lax.rsqrt(jnp.mean(centered * centered, axis=0, keepdims=True) + epsilon)
    return centered * inverse, inverse


def lane_fold(x):
    out = x[:, :CH]
    for m in range(1, x.shape[1] // CH):
        out = out + x[:, m * CH : (m + 1) * CH]
    return out


def peers_of(s):
    return s >> 3, s & 7


def unfold(rows):
    n = rows.shape[0]
    lane = lax.broadcasted_iota(jnp.int32, (n, 128), 1)
    out = []
    for k in range(8):
        at = k * TALL
        m, off = at // 128, at % 128
        v = rows[:, m * 128 : (m + 1) * 128]
        if off + TALL > 128:
            v = jnp.where(lane >= off, v, rows[:, (m + 1) * 128 : (m + 2) * 128])
        out.append(pltpu.roll(v, 128 - off, 1) if off else v)
    return out


def fold(pieces):
    n = pieces[0].shape[0]
    lane = lax.broadcasted_iota(jnp.int32, (n, 128), 1)
    r = [pltpu.roll(p, (k * TALL) % 128, 1) if k else p for k, p in enumerate(pieces)]
    cols = []
    for m in range(STEP // 128):
        lo, hi = m * 128, (m + 1) * 128
        v = None
        for k in range(8):
            a, b = max(lo, k * TALL), min(hi, (k + 1) * TALL)
            if a >= b:
                continue
            v = r[k] if v is None else jnp.where(lane >= a - lo, r[k], v)
        cols.append(v)
    return jnp.concatenate(cols, axis=1)


def sides(w):
    gates = jnp.concatenate([w[:, :CH], w[:, 2 * CH : 3 * CH]], axis=1)
    values = jnp.concatenate([w[:, CH : 2 * CH], w[:, 3 * CH :]], axis=1)
    return gates, values


def k1(crop_ref, pair_ref, ig_ref, ib_ref, w_ref, f_ref, w_s, v_s):
    g = pl.program_id(0)

    @pl.when(g == 0)
    def _():
        perm = interleave()
        gates, values = sides(w_ref[...])
        w_s[: 2 * CH, :] = (0.5 * mm(perm, gates, 1, 1)).astype(bf16)
        w_s[2 * CH :, :] = (0.5 * mm(perm, values, 1, 1)).astype(bf16)
        v_s[0] = column(ig_ref[...])
        v_s[1] = column(ib_ref[...])

    x = turned(pair_ref)
    live = live_cells(crop_ref, g)
    for lo in range(0, STEP, 256):
        hi = min(lo + 256, STEP)
        reps = (hi - lo) // CH
        gain, bias = (jnp.concatenate([v_s[n]] * reps, axis=1) for n in range(2))
        hat, _ = hat_of(x[:, lo:hi])
        normed = (hat * gain + bias).astype(bf16)
        both = mm(w_s[...], normed, 1, 0)
        factor = (jnp.tanh(both[: 2 * CH]) + 1.0) * (both[2 * CH :] * live[:, lo:hi])
        f_ref[:, :, lo:hi] = factor.astype(bf16).reshape(PEERS, 2 * OWN, hi - lo)


def k1b(
    crop_ref, pair_ref, cot_ref, ig_ref, ib_ref, w_ref, gw_ref, n_ref, do_ref, e_ref, sv_ref, sg_ref,
    wg_s, wv_s, gw_s, v_s,
):
    g = pl.program_id(0)

    @pl.when(g == 0)
    def _():
        perm = interleave()
        gates, values = sides(w_ref[...])
        wg_s[...] = mm(perm, gates, 1, 1).astype(bf16)
        wv_s[...] = mm(perm, values, 1, 1).astype(bf16)
        gw_s[...] = gw_ref[...].astype(f32).T.astype(bf16)
        v_s[0] = column(ig_ref[...])
        v_s[1] = column(ib_ref[...])

    hat, _ = hat_of(turned(pair_ref))
    normed = (hat * wide(v_s[0]) + wide(v_s[1])).astype(bf16)
    n_ref[:CH, :] = normed
    n_ref[CH:, :] = jnp.ones((16, STEP), bf16)
    sig = sigmoid(mm(wg_s[...], normed, 1, 0))
    live_sig = sig * live_cells(crop_ref, g)
    sv_ref[...] = live_sig.astype(bf16)
    sg_ref[...] = (live_sig * mm(wv_s[...], normed, 1, 0) * (1.0 - sig)).astype(bf16)
    gate = sigmoid(mm(gw_s[...], normed, 1, 0))
    up = turned(cot_ref) * gate
    do_ref[...] = up.astype(bf16)
    e_ref[...] = up * (1.0 - gate)


def k2(y_ref, _, l_ref, r_ref, z_ref, x_s, p_s, l_s, r_s, sem):
    def spread(s, carry):
        r, c = peers_of(s)
        rows = y_ref[s].astype(f32)
        for g in range(STEPS):
            for k, v in enumerate(unfold(rows[:, g * STEP : (g + 1) * STEP])):
                x_s[r, pl.ds(c * WIDE + g * 8 + k, 2 * OWN, stride=PITCH), :] = v
        return carry

    lax.fori_loop(0, PEERS, spread, 0, unroll=8)
    lane = lax.broadcasted_iota(jnp.int32, (FULL, 128), 1)

    def matrix(t):
        parts = [jnp.where(lane < TALL, x_s[r, t * PITCH : t * PITCH + FULL, :], 0.0) for r in range(ROWS)]
        return jnp.concatenate(parts, axis=1)

    for h in range(OWN):
        left = matrix(h).astype(bf16)
        right = matrix(OWN + h)
        l_s[h] = left
        r_s[h] = right.astype(bf16)
        product = mm(right.T.astype(bf16), left, 1, 0)
        for r in range(ROWS):
            p_s[r, h * JPITCH : h * JPITCH + ROWS * 128, :] = product[:, r * 128 : (r + 1) * 128]

    copies = [pltpu.make_async_copy(l_s, l_ref, sem.at[0]), pltpu.make_async_copy(r_s, r_ref, sem.at[1])]
    for copy in copies:
        copy.start()

    def gather(s, carry):
        r, c = peers_of(s)
        first = (c >> 1) * 128 + (c & 1) * WIDE
        for g in range(STEPS):
            pieces = [p_s[r, pl.ds(first + g * 8 + k, OWN, stride=JPITCH), :] for k in range(8)]
            z_ref[s, :, g * STEP : (g + 1) * STEP] = fold(pieces).astype(bf16)
        return carry

    lax.fori_loop(0, PEERS, gather, 0, unroll=8)
    for copy in copies:
        copy.wait()


def k3(z_ref, do_ref, og_ref, ow_ref, dp_ref, z_s, v_s):
    @pl.when(pl.program_id(0) == 0)
    def _():
        v_s[...] = column(og_ref[...])

    for d in range(PEERS):
        z_s[d * OWN : (d + 1) * OWN, :] = z_ref[d].astype(f32)
    hat, inverse = hat_of(z_s[...])
    scaled = mm(ow_ref[...], do_ref[...], 1, 0) * wide(v_s[...])
    m1 = jnp.mean(scaled, axis=0, keepdims=True)
    m2 = jnp.mean(scaled * hat, axis=0, keepdims=True)
    z_s[...] = inverse * (scaled - m1 - hat * m2)
    for d in range(PEERS):
        dp_ref[d] = z_s[d * OWN : (d + 1) * OWN, :].astype(bf16)


def k3b(
    z_ref, n_ref, do_ref, e_ref, og_ref, ob_ref, ow_ref, dg_ref, gow_ref, gv_ref, gg_ref,
    z_s, owt_s, v_s,
):
    @pl.when(pl.program_id(0) == 0)
    def _():
        owt_s[...] = ow_ref[...].astype(f32).T.astype(bf16)
        v_s[0] = column(og_ref[...])
        v_s[1] = column(ob_ref[...])
        gow_ref[...] = jnp.zeros_like(gow_ref)
        gv_ref[...] = jnp.zeros_like(gv_ref)
        gg_ref[...] = jnp.zeros_like(gg_ref)

    for d in range(PEERS):
        z_s[d * OWN : (d + 1) * OWN, :] = z_ref[d].astype(f32)
    hat, _ = hat_of(z_s[...])
    tri = (hat * wide(v_s[0]) + wide(v_s[1])).astype(bf16)
    d_out = do_ref[...]
    d_gate = (e_ref[...] * mm(owt_s[...], tri, 1, 0)).astype(bf16)
    dg_ref[...] = d_gate
    gow_ref[...] += mm(tri, d_out, 1, 1)
    gg_ref[...] += mm(n_ref[...], d_gate, 1, 1)
    up = mm(ow_ref[...], d_out, 1, 0)
    gv_ref[0] += lane_fold(up * hat)
    gv_ref[1] += lane_fold(up)


def k4(dp_ref, l_ref, r_ref, _, a_ref, x_s, o_s, l_s, r_s, sem):
    copies = [pltpu.make_async_copy(l_ref, l_s, sem.at[0]), pltpu.make_async_copy(r_ref, r_s, sem.at[1])]
    for copy in copies:
        copy.start()
    zero = jnp.zeros((128 - TALL, 128), f32)
    for r in range(ROWS):
        for h in range(OWN):
            for q in range(ROWS):
                at = h * JPITCH + q * 128 + TALL
                x_s[r, at : at + 128 - TALL, :] = zero

    def spread(s, carry):
        r, c = peers_of(s)
        first = (c >> 1) * 128 + (c & 1) * WIDE
        rows = dp_ref[s].astype(f32)
        for g in range(STEPS):
            for k, v in enumerate(unfold(rows[:, g * STEP : (g + 1) * STEP])):
                x_s[r, pl.ds(first + g * 8 + k, OWN, stride=JPITCH), :] = v
        return carry

    lax.fori_loop(0, PEERS, spread, 0, unroll=16)
    for copy in copies:
        copy.wait()
    lane = lax.broadcasted_iota(jnp.int32, (ROWS * 128, 128), 1)
    for h in range(OWN):
        parts = []
        for r in range(ROWS):
            x = x_s[r, h * JPITCH : h * JPITCH + ROWS * 128, :]
            parts.append(jnp.where(lane < TALL, x, 0.0).astype(bf16))
        dp = jnp.concatenate(parts, axis=1)
        d_left = mm(r_s[h], dp, 1, 0)
        d_right = mm(l_s[h], dp, 1, 1)
        for r in range(ROWS):
            o_s[r, h * PITCH : h * PITCH + FULL, :] = d_left[:, r * 128 : (r + 1) * 128]
            at = (OWN + h) * PITCH
            o_s[r, at : at + FULL, :] = d_right[:, r * 128 : (r + 1) * 128]

    def gather(s, carry):
        r, c = peers_of(s)
        for g in range(STEPS):
            pieces = [o_s[r, pl.ds(c * WIDE + g * 8 + k, 2 * OWN, stride=PITCH), :] for k in range(8)]
            a_ref[s, :, g * STEP : (g + 1) * STEP] = fold(pieces).astype(bf16)
        return carry

    lax.fori_loop(0, PEERS, gather, 0, unroll=16)


def k5(
    a_ref, sv_ref, sg_ref, n_ref, ig_ref, ib_ref, w_ref, gw_ref, gow_ref, gv_ref, gg_ref,
    s_ref, ag_s, pk_s,
):
    g = pl.program_id(0)

    @pl.when(g == 0)
    def _():
        ag_s[...] = jnp.zeros_like(ag_s)

    d = a_ref[...].reshape(2 * CH, STEP).astype(f32)
    d_gates = (d * sg_ref[...].astype(f32)).astype(bf16)
    d_values = (d * sv_ref[...].astype(f32)).astype(bf16)
    ag_s[...] += mm(jnp.concatenate([d_gates, d_values], axis=0), n_ref[...], 1, 1)

    @pl.when(g == STEPS - 1)
    def _():
        perm = interleave()
        gates, values = sides(w_ref[...])
        g_gates, g_values = ag_s[: 2 * CH, :].T, ag_s[2 * CH :, :].T
        weights = (mm(gates, perm, 1, 1), mm(values, perm, 1, 1), gw_ref[...].astype(f32))
        slope = jnp.zeros((CH, 1), f32)
        shift = jnp.zeros((CH, 1), f32)
        for weight, grad in zip(weights, (g_gates, g_values, gg_ref[...])):
            slope += jnp.sum(weight * grad[:CH, :], axis=1, keepdims=True)
            shift += jnp.sum(weight * grad[CH : CH + 1, :], axis=1, keepdims=True)
        gain, bias = column(ig_ref[...]), column(ib_ref[...])
        lane = lax.broadcasted_iota(jnp.int32, (CH, CH), 1)
        sums = jnp.where(lane == 0, (slope - bias * shift) / gain, jnp.where(lane == 1, shift, 0.0))
        for n in range(2):
            sums = jnp.where(lane == 2 + n, jnp.sum(gv_ref[n], axis=1, keepdims=True), sums)
        d_gates = mm(g_gates[:CH, :].astype(bf16), perm, 1, 0)
        d_values = mm(g_values[:CH, :].astype(bf16), perm, 1, 0)
        planes = (
            d_gates[:, :CH], d_values[:, :CH], d_gates[:, CH:], d_values[:, CH:],
            gg_ref[:CH, :], gow_ref[...], sums, jnp.zeros((CH, CH), f32),
        )
        for n, plane in enumerate(planes):
            pk_s[pl.ds(n, CH, stride=8), :] = plane
        s_ref[...] = pk_s[...].astype(bf16).reshape(CH, 8, CH)


def k5b(pair_ref, a_ref, sv_ref, sg_ref, dg_ref, ig_ref, w_ref, gw_ref, gp_ref, bk_s, v_s):
    @pl.when(pl.program_id(0) == 0)
    def _():
        perm = interleave()
        gates, values = sides(w_ref[...])
        bk_s[:, : 2 * CH] = mm(gates, perm, 1, 1).astype(bf16)
        bk_s[:, 2 * CH : 4 * CH] = mm(values, perm, 1, 1).astype(bf16)
        bk_s[:, 4 * CH :] = gw_ref[...]
        v_s[...] = column(ig_ref[...])

    hat, inverse = hat_of(turned(pair_ref))
    d = a_ref[...].reshape(2 * CH, STEP).astype(f32)
    d_gates = (d * sg_ref[...].astype(f32)).astype(bf16)
    d_values = (d * sv_ref[...].astype(f32)).astype(bf16)
    d_normed = mm(bk_s[...], jnp.concatenate([d_gates, d_values, dg_ref[...]], axis=0), 1, 0)
    scaled = d_normed * wide(v_s[...])
    m1 = jnp.mean(scaled, axis=0, keepdims=True)
    m2 = jnp.mean(scaled * hat, axis=0, keepdims=True)
    back = (inverse * (scaled - m1 - hat * m2)).T
    flat = gp_ref.reshape(STEP, CH)
    for k in range(8):
        flat[pl.ds(k, TALL, stride=8), :] = back[k * TALL : (k + 1) * TALL, :]


def k6(x_ref, o_ref):
    total = jnp.sum(x_ref[...].astype(f32), axis=0).astype(bf16)
    o_ref[...] = jnp.broadcast_to(total[None], o_ref.shape)


def k7(x_ref, gp_ref, gg_ref, gow_ref, *rest, factor):
    s_s = rest[-1]
    s_s[...] = x_ref[...].astype(f32).reshape(CH * 8, CH) * factor
    for q in range(4):
        gp_ref[:, q * CH : (q + 1) * CH] = s_s[pl.ds(q, CH, stride=8), :]
    gg_ref[...] = s_s[pl.ds(4, CH, stride=8), :]
    gow_ref[...] = s_s[pl.ds(5, CH, stride=8), :]
    sums = s_s[pl.ds(6, CH, stride=8), :].T
    for n in range(4):
        rest[n][...] = sums[n : n + 1]


def whole(*shape):
    return pl.BlockSpec(shape, lambda g: (0,) * len(shape))


def tile():
    return pl.BlockSpec((TALL, 8, CH), lambda g: (0, g, 0))


def lanes(*shape):
    return pl.BlockSpec((*shape, STEP), lambda g: (0,) * len(shape) + (g,))


SMEM = pl.BlockSpec(memory_space=pltpu.SMEM)
SMALL = pltpu.CompilerParams(vmem_limit_bytes=12 << 20)
LARGE = pltpu.CompilerParams(vmem_limit_bytes=22 << 20)
cost = pl.CostEstimate(flops=1_000_000_000, transcendentals=0, bytes_accessed=8_000_000)


def out(shape, dtype):
    return jax.ShapeDtypeStruct(shape, dtype)


def away(shape, dtype):
    return pltpu.HBM(shape, dtype)


def keep_away(*arrays):
    return [pltpu.with_memory_space_constraint(a, pltpu.HBM) for a in arrays]


def vm(*shape, dtype=f32):
    return pltpu.VMEM(shape, dtype)


HERE = pl.BlockSpec(memory_space=pltpu.VMEM)
AWAY = pl.BlockSpec(memory_space=pltpu.HBM)
KEPT = (OWN, FULL, ROWS * 128)


def product_call(factors, after, name):
    return pl.pallas_call(
        k2,
        name=name,
        compiler_params=LARGE,
        in_specs=[HERE, AWAY],
        out_specs=[AWAY, AWAY, HERE],
        out_shape=[away(KEPT, bf16), away(KEPT, bf16), out((PEERS, OWN, CELLS), bf16)],
        scratch_shapes=[
            vm(ROWS, 2 * OWN * PITCH, 128), vm(ROWS, OWN * JPITCH, 128),
            vm(*KEPT, dtype=bf16), vm(*KEPT, dtype=bf16), pltpu.SemaphoreType.DMA((2,)),
        ],
    )(factors, *keep_away(after))


def slopes_call(d_product, left, right, after, name):
    return pl.pallas_call(
        k4,
        name=name,
        compiler_params=LARGE,
        in_specs=[HERE, AWAY, AWAY, AWAY],
        out_specs=HERE,
        out_shape=out((PEERS, 2 * OWN, CELLS), bf16),
        scratch_shapes=[
            vm(ROWS, OWN * JPITCH, 128), vm(ROWS, 2 * OWN * PITCH, 128),
            vm(*KEPT, dtype=bf16), vm(*KEPT, dtype=bf16), pltpu.SemaphoreType.DMA((2,)),
        ],
    )(d_product, *keep_away(left, right, after))


def per_device(
    pair,
    cotangent,
    crop_length,
    in_gain,
    in_bias,
    proj_weight,
    gate_weight,
    out_gain,
    out_bias,
    out_weight,
):
    group = ("row", "col")
    everyone = ("samp", "row", "col")
    swap = functools.partial(lax.all_to_all, split_axis=0, concat_axis=0, tiled=True)
    row = lambda v: v.reshape(1, CH)
    wb = functools.partial(vm, dtype=bf16)
    pair, cotangent = pair[0], cotangent[0]
    in_gain, in_bias, out_gain, out_bias = map(row, (in_gain, in_bias, out_gain, out_bias))
    one, square, proj = whole(1, CH), whole(CH, CH), whole(CH, 4 * CH)
    both = (PEERS, 2 * OWN, CELLS)
    factors = pl.pallas_call(
        k1,
        name="factors",
        compiler_params=SMALL,
        grid=(STEPS,),
        in_specs=[SMEM, tile(), one, one, proj],
        out_specs=lanes(PEERS, 2 * OWN),
        out_shape=out(both, bf16),
        scratch_shapes=[wb(4 * CH, CH), vm(2, CH, CH)],
    )(crop_length, *keep_away(pair, in_gain, in_bias, proj_weight))
    factors = swap(factors, group)
    normed, d_out, slope, by_value, by_gate = pl.pallas_call(
        k1b,
        name="gate",
        compiler_params=SMALL,
        grid=(STEPS,),
        in_specs=[SMEM, tile(), tile(), one, one, proj, square],
        out_specs=[lanes(CH + 16), lanes(CH), lanes(CH), lanes(2 * CH), lanes(2 * CH)],
        out_shape=[
            away((CH + 16, CELLS), bf16), away((CH, CELLS), bf16), away((CH, CELLS), f32),
            away((2 * CH, CELLS), bf16), away((2 * CH, CELLS), bf16),
        ],
        scratch_shapes=[wb(2 * CH, CH), wb(2 * CH, CH), wb(CH, CH), vm(2, CH, CH)],
        cost_estimate=cost,
    )(crop_length, *keep_away(pair, cotangent, in_gain, in_bias, proj_weight, gate_weight))
    left, right, product = product_call(factors, d_out, "product")
    product = swap(product, group)
    d_product = pl.pallas_call(
        k3,
        name="middle",
        compiler_params=SMALL,
        grid=(STEPS,),
        in_specs=[lanes(PEERS, OWN), lanes(CH), one, square],
        out_specs=lanes(PEERS, OWN),
        out_shape=out((PEERS, OWN, CELLS), bf16),
        scratch_shapes=[vm(CH, STEP), vm(CH, CH)],
    )(product, d_out, out_gain, out_weight)
    d_product = swap(d_product, group)
    d_gate, g_out_weight, g_out, g_gate = pl.pallas_call(
        k3b,
        name="outputs",
        compiler_params=SMALL,
        grid=(STEPS,),
        in_specs=[lanes(PEERS, OWN), lanes(CH + 16), lanes(CH), lanes(CH), one, one, square],
        out_specs=[lanes(CH), square, whole(2, CH, CH), whole(CH + 16, CH)],
        out_shape=[
            away((CH, CELLS), bf16), away((CH, CH), f32), away((2, CH, CH), f32), away((CH + 16, CH), f32),
        ],
        scratch_shapes=[vm(CH, STEP), wb(CH, CH), vm(2, CH, CH)],
        cost_estimate=cost,
    )(product, *keep_away(normed, d_out, slope, out_gain, out_bias, out_weight))
    d_factors = slopes_call(d_product, left, right, d_gate, "slopes")
    d_factors = swap(d_factors, group)
    packed = pl.pallas_call(
        k5,
        name="weights",
        compiler_params=SMALL,
        grid=(STEPS,),
        in_specs=[
            lanes(PEERS, 2 * OWN), lanes(2 * CH), lanes(2 * CH), lanes(CH + 16), one, one,
            proj, square, square, whole(2, CH, CH), whole(CH + 16, CH),
        ],
        out_specs=whole(CH, 8, CH),
        out_shape=out((CH, 8, CH), bf16),
        scratch_shapes=[vm(4 * CH, CH + 16), vm(CH * 8, CH)],
    )(d_factors, by_value, by_gate, normed, in_gain, in_bias, proj_weight, gate_weight,
      g_out_weight, g_out, g_gate)
    parts = swap(packed, everyone)
    grad_pair = pl.pallas_call(
        k5b,
        name="inputs",
        compiler_params=SMALL,
        grid=(STEPS,),
        in_specs=[
            tile(), lanes(PEERS, 2 * OWN), lanes(2 * CH), lanes(2 * CH), lanes(CH), one, proj, square,
        ],
        out_specs=tile(),
        out_shape=out((TALL, WIDE, CH), f32),
        scratch_shapes=[wb(CH, 5 * CH), vm(CH, CH)],
        cost_estimate=cost,
    )(*keep_away(pair), d_factors, *keep_away(by_value, by_gate, d_gate, in_gain, proj_weight, gate_weight))
    total = pl.pallas_call(k6, name="total", compiler_params=SMALL, out_shape=out((CH, 8, CH), bf16))(parts)
    total = swap(total, everyone)
    g_proj_weight, g_gate_weight, g_out_weight, *sums = pl.pallas_call(
        functools.partial(k7, factor=1.0 / FULL),
        name="unpack",
        compiler_params=SMALL,
        out_shape=[out((CH, 4 * CH), f32), out((CH, CH), f32), out((CH, CH), f32)] + [out((1, CH), f32)] * 4,
        scratch_shapes=[vm(CH * 8, CH)],
    )(total)
    sums = [s.reshape(CH) for s in sums]
    return (
        grad_pair[None],
        sums[0],
        sums[1],
        g_proj_weight,
        g_gate_weight,
        sums[2],
        sums[3],
        g_out_weight,
    )


def solution(mesh):
    return jax.shard_map(
        per_device,
        mesh=mesh,
        in_specs=(
            P("samp", "row", "col", None),
            P("samp", "row", "col", None),
            P("samp"),
            P(),
            P(),
            P(),
            P(),
            P(),
            P(),
            P(),
        ),
        out_specs=(P("samp", "row", "col", None), P(), P(), P(), P(), P(), P(), P()),
        check_vma=False,
    )
```

```python
import functools

import jax
import jax.numpy as jnp
from jax import lax
from jax.experimental import pallas as pl
from jax.experimental.pallas import tpu as pltpu
from jax.sharding import PartitionSpec as P

epsilon = 1e-05

TALL = 80
WIDE = 40
CH = 128
ROWS = 4
COLS = 8
PEERS = ROWS * COLS
OWN = CH // PEERS
CELLS = TALL * WIDE
STEP = 8 * TALL
STEPS = CELLS // STEP
FULL = COLS * WIDE
PITCH = FULL + 8
JPITCH = ROWS * 128 + 8
f32 = jnp.float32
bf16 = jnp.bfloat16


def mm(a, b, ca, cb):
    return lax.dot_general(a, b, (((ca,), (cb,)), ((), ())), preferred_element_type=f32)


def sigmoid(x):
    return 0.5 * jnp.tanh(0.5 * x) + 0.5


def column(row):
    return jnp.broadcast_to(row, (CH, CH)).T


def wide(col):
    return jnp.concatenate([col] * (STEP // CH), axis=1)


def interleave():
    n = 2 * CH
    q = lax.broadcasted_iota(jnp.int32, (n, n), 0)
    p = lax.broadcasted_iota(jnp.int32, (n, n), 1)
    src = ((q >> 2) & 1) * CH + (q >> 3) * OWN + (q & 3)
    return jnp.where(src == p, 1.0, 0.0).astype(bf16)


def turned(ref):
    flat = ref.reshape(STEP, CH)
    rows = [flat[pl.ds(k, TALL, stride=8), :] for k in range(8)]
    return jnp.concatenate(rows, axis=0).T


def live_cells(crop_ref, g):
    lane = lax.broadcasted_iota(jnp.int32, (1, STEP), 1)
    k = jnp.zeros((1, STEP), jnp.int32)
    for m in range(1, 8):
        k = k + jnp.where(lane >= m * TALL, 1, 0)
    i = lane - k * TALL + lax.axis_index("row") * TALL
    k = k + (g * 8 + lax.axis_index("col") * WIDE)
    live = jnp.logical_and(i < crop_ref[0], k < crop_ref[0])
    return jnp.where(live, 1.0, 0.0).astype(f32)


def hat_of(x):
    centre = jnp.mean(x, axis=0, keepdims=True)
    centered = x - centre
    inverse = lax.rsqrt(jnp.mean(centered * centered, axis=0, keepdims=True) + epsilon)
    return centered * inverse, inverse


def lane_fold(x):
    out = x[:, :CH]
    for m in range(1, x.shape[1] // CH):
        out = out + x[:, m * CH : (m + 1) * CH]
    return out


def peers_of(s):
    return s >> 3, s & 7


def unfold(rows):
    n = rows.shape[0]
    lane = lax.broadcasted_iota(jnp.int32, (n, 128), 1)
    out = []
    for k in range(8):
        at = k * TALL
        m, off = at // 128, at % 128
        v = rows[:, m * 128 : (m + 1) * 128]
        if off + TALL > 128:
            v = jnp.where(lane >= off, v, rows[:, (m + 1) * 128 : (m + 2) * 128])
        out.append(pltpu.roll(v, 128 - off, 1) if off else v)
    return out


def fold(pieces):
    n = pieces[0].shape[0]
    lane = lax.broadcasted_iota(jnp.int32, (n, 128), 1)
    r = [pltpu.roll(p, (k * TALL) % 128, 1) if k else p for k, p in enumerate(pieces)]
    cols = []
    for m in range(STEP // 128):
        lo, hi = m * 128, (m + 1) * 128
        v = None
        for k in range(8):
            a, b = max(lo, k * TALL), min(hi, (k + 1) * TALL)
            if a >= b:
                continue
            v = r[k] if v is None else jnp.where(lane >= a - lo, r[k], v)
        cols.append(v)
    return jnp.concatenate(cols, axis=1)


def sides(w):
    gates = jnp.concatenate([w[:, :CH], w[:, 2 * CH : 3 * CH]], axis=1)
    values = jnp.concatenate([w[:, CH : 2 * CH], w[:, 3 * CH :]], axis=1)
    return gates, values


def k1(crop_ref, pair_ref, ig_ref, ib_ref, w_ref, f_ref, w_s, v_s):
    g = pl.program_id(0)

    @pl.when(g == 0)
    def _():
        perm = interleave()
        gates, values = sides(w_ref[...])
        w_s[: 2 * CH, :] = (0.5 * mm(perm, gates, 1, 1)).astype(bf16)
        w_s[2 * CH :, :] = (0.5 * mm(perm, values, 1, 1)).astype(bf16)
        v_s[0] = column(ig_ref[...])
        v_s[1] = column(ib_ref[...])

    x = turned(pair_ref)
    live = live_cells(crop_ref, g)
    for lo in range(0, STEP, 256):
        hi = min(lo + 256, STEP)
        reps = (hi - lo) // CH
        gain, bias = (jnp.concatenate([v_s[n]] * reps, axis=1) for n in range(2))
        hat, _ = hat_of(x[:, lo:hi])
        normed = (hat * gain + bias).astype(bf16)
        both = mm(w_s[...], normed, 1, 0)
        factor = (jnp.tanh(both[: 2 * CH]) + 1.0) * (both[2 * CH :] * live[:, lo:hi])
        f_ref[:, :, lo:hi] = factor.astype(bf16).reshape(PEERS, 2 * OWN, hi - lo)


def k1b(
    crop_ref, pair_ref, cot_ref, ig_ref, ib_ref, w_ref, gw_ref, n_ref, do_ref, e_ref, sv_ref, sg_ref,
    wg_s, wv_s, gw_s, v_s,
):
    g = pl.program_id(0)

    @pl.when(g == 0)
    def _():
        perm = interleave()
        gates, values = sides(w_ref[...])
        wg_s[...] = mm(perm, gates, 1, 1).astype(bf16)
        wv_s[...] = mm(perm, values, 1, 1).astype(bf16)
        gw_s[...] = gw_ref[...].astype(f32).T.astype(bf16)
        v_s[0] = column(ig_ref[...])
        v_s[1] = column(ib_ref[...])

    hat, _ = hat_of(turned(pair_ref))
    normed = (hat * wide(v_s[0]) + wide(v_s[1])).astype(bf16)
    n_ref[:CH, :] = normed
    n_ref[CH:, :] = jnp.ones((16, STEP), bf16)
    sig = sigmoid(mm(wg_s[...], normed, 1, 0))
    live_sig = sig * live_cells(crop_ref, g)
    sv_ref[...] = live_sig.astype(bf16)
    sg_ref[...] = (live_sig * mm(wv_s[...], normed, 1, 0) * (1.0 - sig)).astype(bf16)
    gate = sigmoid(mm(gw_s[...], normed, 1, 0))
    up = turned(cot_ref) * gate
    do_ref[...] = up.astype(bf16)
    e_ref[...] = up * (1.0 - gate)


def k2(y_ref, _, l_ref, r_ref, z_ref, x_s, p_s, l_s, r_s, sem):
    def spread(s, carry):
        r, c = peers_of(s)
        rows = y_ref[s].astype(f32)
        for g in range(STEPS):
            for k, v in enumerate(unfold(rows[:, g * STEP : (g + 1) * STEP])):
                x_s[r, pl.ds(c * WIDE + g * 8 + k, 2 * OWN, stride=PITCH), :] = v
        return carry

    lax.fori_loop(0, PEERS, spread, 0, unroll=8)
    lane = lax.broadcasted_iota(jnp.int32, (FULL, 128), 1)

    def matrix(t):
        parts = [jnp.where(lane < TALL, x_s[r, t * PITCH : t * PITCH + FULL, :], 0.0) for r in range(ROWS)]
        return jnp.concatenate(parts, axis=1)

    for h in range(OWN):
        left = matrix(h).astype(bf16)
        right = matrix(OWN + h).astype(bf16)
        l_s[h] = left
        r_s[h] = right
        product = mm(right, left, 0, 0)
        for r in range(ROWS):
            p_s[r, h * JPITCH : h * JPITCH + ROWS * 128, :] = product[:, r * 128 : (r + 1) * 128]

    copies = [pltpu.make_async_copy(l_s, l_ref, sem.at[0]), pltpu.make_async_copy(r_s, r_ref, sem.at[1])]
    for copy in copies:
        copy.start()

    def gather(s, carry):
        r, c = peers_of(s)
        first = (c >> 1) * 128 + (c & 1) * WIDE
        for g in range(STEPS):
            pieces = [p_s[r, pl.ds(first + g * 8 + k, OWN, stride=JPITCH), :] for k in range(8)]
            z_ref[s, :, g * STEP : (g + 1) * STEP] = fold(pieces).astype(bf16)
        return carry

    lax.fori_loop(0, PEERS, gather, 0, unroll=8)
    for copy in copies:
        copy.wait()


def k3(z_ref, do_ref, og_ref, ow_ref, dp_ref, z_s, b_s, sem):
    gain = wide(column(og_ref[...]))
    copies = []
    for g in range(STEPS):
        at = pl.ds(g * STEP, STEP)
        for d in range(PEERS):
            z_s[g, d * OWN : (d + 1) * OWN, :] = z_ref[d, :, at].astype(f32)
        hat, inverse = hat_of(z_s[g])
        scaled = mm(ow_ref[...], do_ref[:, at], 1, 0) * gain
        m1 = jnp.mean(scaled, axis=0, keepdims=True)
        m2 = jnp.mean(scaled * hat, axis=0, keepdims=True)
        z_s[g] = inverse * (scaled - m1 - hat * m2)
        for d in range(PEERS):
            b_s[d, :, at] = z_s[g, d * OWN : (d + 1) * OWN, :].astype(bf16)
        if copies:
            copies[-1].start()
        copies.append(pltpu.make_async_copy(b_s.at[:, :, at], dp_ref.at[:, :, at], sem.at[g]))
    copies[-1].start()
    for copy in copies:
        copy.wait()


def k3b(
    z_ref, n_ref, do_ref, e_ref, og_ref, ob_ref, ow_ref, dg_ref, gow_ref, gv_ref, gg_ref,
    z_s, owt_s, v_s,
):
    @pl.when(pl.program_id(0) == 0)
    def _():
        owt_s[...] = ow_ref[...].astype(f32).T.astype(bf16)
        v_s[0] = column(og_ref[...])
        v_s[1] = column(ob_ref[...])
        gow_ref[...] = jnp.zeros_like(gow_ref)
        gv_ref[...] = jnp.zeros_like(gv_ref)
        gg_ref[...] = jnp.zeros_like(gg_ref)

    for d in range(PEERS):
        z_s[d * OWN : (d + 1) * OWN, :] = z_ref[d].astype(f32)
    hat, _ = hat_of(z_s[...])
    tri = (hat * wide(v_s[0]) + wide(v_s[1])).astype(bf16)
    d_out = do_ref[...]
    d_gate = (e_ref[...] * mm(owt_s[...], tri, 1, 0)).astype(bf16)
    dg_ref[...] = d_gate
    gow_ref[...] += mm(tri, d_out, 1, 1)
    gg_ref[...] += mm(n_ref[...], d_gate, 1, 1)
    up = mm(ow_ref[...], d_out, 1, 0)
    gv_ref[0] += lane_fold(up * hat)
    gv_ref[1] += lane_fold(up)


def k4(dp_ref, l_ref, r_ref, _, a_ref, x_s, o_s, l_s, r_s, sem):
    copies = [pltpu.make_async_copy(l_ref, l_s, sem.at[0]), pltpu.make_async_copy(r_ref, r_s, sem.at[1])]
    for copy in copies:
        copy.start()
    zero = jnp.zeros((128 - TALL, 128), f32)
    for r in range(ROWS):
        for h in range(OWN):
            for q in range(ROWS):
                at = h * JPITCH + q * 128 + TALL
                x_s[r, at : at + 128 - TALL, :] = zero

    def spread(s, carry):
        r, c = peers_of(s)
        first = (c >> 1) * 128 + (c & 1) * WIDE
        rows = dp_ref[s].astype(f32)
        for g in range(STEPS):
            for k, v in enumerate(unfold(rows[:, g * STEP : (g + 1) * STEP])):
                x_s[r, pl.ds(first + g * 8 + k, OWN, stride=JPITCH), :] = v
        return carry

    lax.fori_loop(0, PEERS, spread, 0, unroll=16)
    for copy in copies:
        copy.wait()
    lane = lax.broadcasted_iota(jnp.int32, (ROWS * 128, 128), 1)
    for h in range(OWN):
        parts = []
        for r in range(ROWS):
            x = x_s[r, h * JPITCH : h * JPITCH + ROWS * 128, :]
            parts.append(jnp.where(lane < TALL, x, 0.0).astype(bf16))
        dp = jnp.concatenate(parts, axis=1)
        d_left = mm(r_s[h], dp, 1, 0)
        d_right = mm(l_s[h], dp, 1, 1)
        for r in range(ROWS):
            o_s[r, h * PITCH : h * PITCH + FULL, :] = d_left[:, r * 128 : (r + 1) * 128]
            at = (OWN + h) * PITCH
            o_s[r, at : at + FULL, :] = d_right[:, r * 128 : (r + 1) * 128]

    def gather(s, carry):
        r, c = peers_of(s)
        for g in range(STEPS):
            pieces = [o_s[r, pl.ds(c * WIDE + g * 8 + k, 2 * OWN, stride=PITCH), :] for k in range(8)]
            a_ref[s, :, g * STEP : (g + 1) * STEP] = fold(pieces).astype(bf16)
        return carry

    lax.fori_loop(0, PEERS, gather, 0, unroll=16)


def k5(
    a_ref, sv_ref, sg_ref, n_ref, ig_ref, ib_ref, w_ref, gw_ref, gow_ref, gv_ref, gg_ref,
    s_ref, ag_s, pk_s,
):
    total = None
    for g in range(STEPS):
        at = slice(g * STEP, (g + 1) * STEP)
        d = a_ref[:, :, at].reshape(2 * CH, STEP)
        slopes = jnp.concatenate([d * sg_ref[:, at], d * sv_ref[:, at]], axis=0)
        part = mm(slopes, n_ref[:, at], 1, 1)
        total = part if total is None else total + part
    ag_s[...] = total
    perm = interleave()
    gates, values = sides(w_ref[...])
    g_gates, g_values = ag_s[: 2 * CH, :].T, ag_s[2 * CH :, :].T
    weights = (mm(gates, perm, 1, 1), mm(values, perm, 1, 1), gw_ref[...].astype(f32))
    slope = jnp.zeros((CH, 1), f32)
    shift = jnp.zeros((CH, 1), f32)
    for weight, grad in zip(weights, (g_gates, g_values, gg_ref[...])):
        slope += jnp.sum(weight * grad[:CH, :], axis=1, keepdims=True)
        shift += jnp.sum(weight * grad[CH : CH + 1, :], axis=1, keepdims=True)
    gain, bias = column(ig_ref[...]), column(ib_ref[...])
    lane = lax.broadcasted_iota(jnp.int32, (CH, CH), 1)
    sums = jnp.where(lane == 0, (slope - bias * shift) / gain, jnp.where(lane == 1, shift, 0.0))
    for n in range(2):
        sums = jnp.where(lane == 2 + n, jnp.sum(gv_ref[n], axis=1, keepdims=True), sums)
    d_gates = mm(g_gates[:CH, :].astype(bf16), perm, 1, 0)
    d_values = mm(g_values[:CH, :].astype(bf16), perm, 1, 0)
    planes = (
        d_gates[:, :CH], d_values[:, :CH], d_gates[:, CH:], d_values[:, CH:],
        gg_ref[:CH, :], gow_ref[...], sums, jnp.zeros((CH, CH), f32),
    )
    for n, plane in enumerate(planes):
        pk_s[pl.ds(n, CH, stride=8), :] = plane
    s_ref[...] = pk_s[...].astype(bf16).reshape(CH, 8, CH)


def k5b(pair_ref, a_ref, sv_ref, sg_ref, dg_ref, ig_ref, w_ref, gw_ref, gp_ref, bk_s, v_s):
    @pl.when(pl.program_id(0) == 0)
    def _():
        perm = interleave()
        gates, values = sides(w_ref[...])
        bk_s[:, : 2 * CH] = mm(gates, perm, 1, 1).astype(bf16)
        bk_s[:, 2 * CH : 4 * CH] = mm(values, perm, 1, 1).astype(bf16)
        bk_s[:, 4 * CH :] = gw_ref[...]
        v_s[...] = column(ig_ref[...])

    hat, inverse = hat_of(turned(pair_ref))
    d = a_ref[...].reshape(2 * CH, STEP).astype(f32)
    d_gates = (d * sg_ref[...].astype(f32)).astype(bf16)
    d_values = (d * sv_ref[...].astype(f32)).astype(bf16)
    d_normed = mm(bk_s[...], jnp.concatenate([d_gates, d_values, dg_ref[...]], axis=0), 1, 0)
    scaled = d_normed * wide(v_s[...])
    m1 = jnp.mean(scaled, axis=0, keepdims=True)
    m2 = jnp.mean(scaled * hat, axis=0, keepdims=True)
    back = (inverse * (scaled - m1 - hat * m2)).T
    flat = gp_ref.reshape(STEP, CH)
    for k in range(8):
        flat[pl.ds(k, TALL, stride=8), :] = back[k * TALL : (k + 1) * TALL, :]


def k6(x_ref, o_ref):
    total = jnp.sum(x_ref[...].astype(f32), axis=0).astype(bf16)
    o_ref[...] = jnp.broadcast_to(total[None], o_ref.shape)


def k7(x_ref, gp_ref, gg_ref, gow_ref, *rest, factor):
    s_s = rest[-1]
    s_s[...] = x_ref[...].astype(f32).reshape(CH * 8, CH) * factor
    for q in range(4):
        gp_ref[:, q * CH : (q + 1) * CH] = s_s[pl.ds(q, CH, stride=8), :]
    gg_ref[...] = s_s[pl.ds(4, CH, stride=8), :]
    gow_ref[...] = s_s[pl.ds(5, CH, stride=8), :]
    sums = s_s[pl.ds(6, CH, stride=8), :].T
    for n in range(4):
        rest[n][...] = sums[n : n + 1]


def whole(*shape):
    return pl.BlockSpec(shape, lambda g: (0,) * len(shape))


def tile():
    return pl.BlockSpec((TALL, 8, CH), lambda g: (0, g, 0))


def lanes(*shape):
    return pl.BlockSpec((*shape, STEP), lambda g: (0,) * len(shape) + (g,))


SMEM = pl.BlockSpec(memory_space=pltpu.SMEM)
SMALL = pltpu.CompilerParams(vmem_limit_bytes=12 << 20)
LARGE = pltpu.CompilerParams(vmem_limit_bytes=22 << 20)
cost = pl.CostEstimate(flops=1_000_000_000, transcendentals=0, bytes_accessed=8_000_000)


def out(shape, dtype):
    return jax.ShapeDtypeStruct(shape, dtype)


def away(shape, dtype):
    return pltpu.HBM(shape, dtype)


def keep_away(*arrays):
    return [pltpu.with_memory_space_constraint(a, pltpu.HBM) for a in arrays]


def vm(*shape, dtype=f32):
    return pltpu.VMEM(shape, dtype)


HERE = pl.BlockSpec(memory_space=pltpu.VMEM)
AWAY = pl.BlockSpec(memory_space=pltpu.HBM)
KEPT = (OWN, FULL, ROWS * 128)


def product_call(factors, after, name):
    return pl.pallas_call(
        k2,
        name=name,
        compiler_params=LARGE,
        in_specs=[HERE, AWAY],
        out_specs=[AWAY, AWAY, HERE],
        out_shape=[away(KEPT, bf16), away(KEPT, bf16), out((PEERS, OWN, CELLS), bf16)],
        scratch_shapes=[
            vm(ROWS, 2 * OWN * PITCH, 128), vm(ROWS, OWN * JPITCH, 128),
            vm(*KEPT, dtype=bf16), vm(*KEPT, dtype=bf16), pltpu.SemaphoreType.DMA((2,)),
        ],
    )(factors, *keep_away(after))


def slopes_call(d_product, left, right, after, name):
    return pl.pallas_call(
        k4,
        name=name,
        compiler_params=LARGE,
        in_specs=[HERE, AWAY, AWAY, AWAY],
        out_specs=HERE,
        out_shape=out((PEERS, 2 * OWN, CELLS), bf16),
        scratch_shapes=[
            vm(ROWS, OWN * JPITCH, 128), vm(ROWS, 2 * OWN * PITCH, 128),
            vm(*KEPT, dtype=bf16), vm(*KEPT, dtype=bf16), pltpu.SemaphoreType.DMA((2,)),
        ],
    )(d_product, *keep_away(left, right, after))


def per_device(
    pair,
    cotangent,
    crop_length,
    in_gain,
    in_bias,
    proj_weight,
    gate_weight,
    out_gain,
    out_bias,
    out_weight,
):
    group = ("row", "col")
    everyone = ("samp", "row", "col")
    swap = functools.partial(lax.all_to_all, split_axis=0, concat_axis=0, tiled=True)
    row = lambda v: v.reshape(1, CH)
    wb = functools.partial(vm, dtype=bf16)
    pair, cotangent = pair[0], cotangent[0]
    in_gain, in_bias, out_gain, out_bias = map(row, (in_gain, in_bias, out_gain, out_bias))
    one, square, proj = whole(1, CH), whole(CH, CH), whole(CH, 4 * CH)
    both = (PEERS, 2 * OWN, CELLS)
    factors = pl.pallas_call(
        k1,
        name="factors",
        compiler_params=SMALL,
        grid=(STEPS,),
        in_specs=[SMEM, tile(), one, one, proj],
        out_specs=lanes(PEERS, 2 * OWN),
        out_shape=out(both, bf16),
        scratch_shapes=[wb(4 * CH, CH), vm(2, CH, CH)],
    )(crop_length, *keep_away(pair, in_gain, in_bias, proj_weight))
    factors = swap(factors, group)
    normed, d_out, slope, by_value, by_gate = pl.pallas_call(
        k1b,
        name="gate",
        compiler_params=SMALL,
        grid=(STEPS,),
        in_specs=[SMEM, tile(), tile(), one, one, proj, square],
        out_specs=[lanes(CH + 16), lanes(CH), lanes(CH), lanes(2 * CH), lanes(2 * CH)],
        out_shape=[
            away((CH + 16, CELLS), bf16), away((CH, CELLS), bf16), away((CH, CELLS), f32),
            away((2 * CH, CELLS), bf16), away((2 * CH, CELLS), bf16),
        ],
        scratch_shapes=[wb(2 * CH, CH), wb(2 * CH, CH), wb(CH, CH), vm(2, CH, CH)],
        cost_estimate=cost,
    )(crop_length, *keep_away(pair, cotangent, in_gain, in_bias, proj_weight, gate_weight))
    left, right, product = product_call(factors, d_out, "product")
    product = swap(product, group)
    d_product = pl.pallas_call(
        k3,
        name="middle",
        compiler_params=SMALL,
        in_specs=[HERE] * 4,
        out_specs=AWAY,
        out_shape=away((PEERS, OWN, CELLS), bf16),
        scratch_shapes=[vm(STEPS, CH, STEP), wb(PEERS, OWN, CELLS), pltpu.SemaphoreType.DMA((STEPS,))],
    )(product, d_out, out_gain, out_weight)
    d_product = swap(d_product, group)
    d_gate, g_out_weight, g_out, g_gate = pl.pallas_call(
        k3b,
        name="outputs",
        compiler_params=SMALL,
        grid=(STEPS,),
        in_specs=[lanes(PEERS, OWN), lanes(CH + 16), lanes(CH), lanes(CH), one, one, square],
        out_specs=[lanes(CH), square, whole(2, CH, CH), whole(CH + 16, CH)],
        out_shape=[
            away((CH, CELLS), bf16), away((CH, CH), f32), away((2, CH, CH), f32), away((CH + 16, CH), f32),
        ],
        scratch_shapes=[vm(CH, STEP), wb(CH, CH), vm(2, CH, CH)],
        cost_estimate=cost,
    )(product, *keep_away(normed, d_out, slope, out_gain, out_bias, out_weight))
    d_factors = slopes_call(d_product, left, right, d_gate, "slopes")
    d_factors = swap(d_factors, group)
    packed = pl.pallas_call(
        k5,
        name="weights",
        compiler_params=SMALL,
        in_specs=[HERE] * 11,
        out_specs=HERE,
        out_shape=out((CH, 8, CH), bf16),
        scratch_shapes=[vm(4 * CH, CH + 16), vm(CH * 8, CH)],
    )(d_factors, by_value, by_gate, normed, in_gain, in_bias, proj_weight, gate_weight,
      g_out_weight, g_out, g_gate)
    parts = swap(packed, everyone)
    grad_pair = pl.pallas_call(
        k5b,
        name="inputs",
        compiler_params=SMALL,
        grid=(STEPS,),
        in_specs=[
            tile(), lanes(PEERS, 2 * OWN), lanes(2 * CH), lanes(2 * CH), lanes(CH), one, proj, square,
        ],
        out_specs=tile(),
        out_shape=out((TALL, WIDE, CH), f32),
        scratch_shapes=[wb(CH, 5 * CH), vm(CH, CH)],
        cost_estimate=cost,
    )(*keep_away(pair), d_factors, *keep_away(by_value, by_gate, d_gate, in_gain, proj_weight, gate_weight))
    total = pl.pallas_call(k6, name="total", compiler_params=SMALL, out_shape=out((CH, 8, CH), bf16))(parts)
    total = swap(total, everyone)
    g_proj_weight, g_gate_weight, g_out_weight, *sums = pl.pallas_call(
        functools.partial(k7, factor=1.0 / FULL),
        name="unpack",
        compiler_params=SMALL,
        out_shape=[out((CH, 4 * CH), f32), out((CH, CH), f32), out((CH, CH), f32)] + [out((1, CH), f32)] * 4,
        scratch_shapes=[vm(CH * 8, CH)],
    )(total)
    sums = [s.reshape(CH) for s in sums]
    return (
        grad_pair[None],
        sums[0],
        sums[1],
        g_proj_weight,
        g_gate_weight,
        sums[2],
        sums[3],
        g_out_weight,
    )


def solution(mesh):
    return jax.shard_map(
        per_device,
        mesh=mesh,
        in_specs=(
            P("samp", "row", "col", None),
            P("samp", "row", "col", None),
            P("samp"),
            P(),
            P(),
            P(),
            P(),
            P(),
            P(),
            P(),
        ),
        out_specs=(P("samp", "row", "col", None), P(), P(), P(), P(), P(), P(), P()),
        check_vma=False,
    )
```

```python
import functools

import jax
import jax.numpy as jnp
from jax import lax
from jax.experimental import pallas as pl
from jax.experimental.pallas import tpu as pltpu
from jax.sharding import PartitionSpec as P

epsilon = 1e-05

TALL = 80
WIDE = 40
CH = 128
ROWS = 4
COLS = 8
PEERS = ROWS * COLS
OWN = CH // PEERS
CELLS = TALL * WIDE
STEP = 8 * TALL
STEPS = CELLS // STEP
FULL = COLS * WIDE
PITCH = FULL + 8
JPITCH = ROWS * 128 + 8
f32 = jnp.float32
bf16 = jnp.bfloat16


def mm(a, b, ca, cb):
    return lax.dot_general(a, b, (((ca,), (cb,)), ((), ())), preferred_element_type=f32)


def sigmoid(x):
    return 0.5 * jnp.tanh(0.5 * x) + 0.5


def column(row):
    return jnp.broadcast_to(row, (CH, CH)).T


def wide(col):
    return jnp.concatenate([col] * (STEP // CH), axis=1)


def interleave():
    n = 2 * CH
    q = lax.broadcasted_iota(jnp.int32, (n, n), 0)
    p = lax.broadcasted_iota(jnp.int32, (n, n), 1)
    src = ((q >> 2) & 1) * CH + (q >> 3) * OWN + (q & 3)
    return jnp.where(src == p, 1.0, 0.0).astype(bf16)


def turned(ref):
    flat = ref.reshape(STEP, CH)
    rows = [flat[pl.ds(k, TALL, stride=8), :] for k in range(8)]
    return jnp.concatenate(rows, axis=0).T


def live_cells(crop_ref, g):
    lane = lax.broadcasted_iota(jnp.int32, (1, STEP), 1)
    k = jnp.zeros((1, STEP), jnp.int32)
    for m in range(1, 8):
        k = k + jnp.where(lane >= m * TALL, 1, 0)
    i = lane - k * TALL + lax.axis_index("row") * TALL
    k = k + (g * 8 + lax.axis_index("col") * WIDE)
    live = jnp.logical_and(i < crop_ref[0], k < crop_ref[0])
    return jnp.where(live, 1.0, 0.0).astype(f32)


def hat_of(x):
    centre = jnp.mean(x, axis=0, keepdims=True)
    centered = x - centre
    inverse = lax.rsqrt(jnp.mean(centered * centered, axis=0, keepdims=True) + epsilon)
    return centered * inverse, inverse


def lane_fold(x):
    out = x[:, :CH]
    for m in range(1, x.shape[1] // CH):
        out = out + x[:, m * CH : (m + 1) * CH]
    return out


def peers_of(s):
    return s >> 3, s & 7


def unfold(rows):
    n = rows.shape[0]
    lane = lax.broadcasted_iota(jnp.int32, (n, 128), 1)
    out = []
    for k in range(8):
        at = k * TALL
        m, off = at // 128, at % 128
        v = rows[:, m * 128 : (m + 1) * 128]
        if off + TALL > 128:
            v = jnp.where(lane >= off, v, rows[:, (m + 1) * 128 : (m + 2) * 128])
        out.append(pltpu.roll(v, 128 - off, 1) if off else v)
    return out


def fold(pieces):
    n = pieces[0].shape[0]
    lane = lax.broadcasted_iota(jnp.int32, (n, 128), 1)
    r = [pltpu.roll(p, (k * TALL) % 128, 1) if k else p for k, p in enumerate(pieces)]
    cols = []
    for m in range(STEP // 128):
        lo, hi = m * 128, (m + 1) * 128
        v = None
        for k in range(8):
            a, b = max(lo, k * TALL), min(hi, (k + 1) * TALL)
            if a >= b:
                continue
            v = r[k] if v is None else jnp.where(lane >= a - lo, r[k], v)
        cols.append(v)
    return jnp.concatenate(cols, axis=1)


def sides(w):
    gates = jnp.concatenate([w[:, :CH], w[:, 2 * CH : 3 * CH]], axis=1)
    values = jnp.concatenate([w[:, CH : 2 * CH], w[:, 3 * CH :]], axis=1)
    return gates, values


def k1(crop_ref, pair_ref, ig_ref, ib_ref, w_ref, f_ref, w_s, v_s):
    g = pl.program_id(0)

    @pl.when(g == 0)
    def _():
        perm = interleave()
        gates, values = sides(w_ref[...])
        w_s[: 2 * CH, :] = (0.5 * mm(perm, gates, 1, 1)).astype(bf16)
        w_s[2 * CH :, :] = (0.5 * mm(perm, values, 1, 1)).astype(bf16)
        v_s[0] = column(ig_ref[...])
        v_s[1] = column(ib_ref[...])

    x = turned(pair_ref)
    live = live_cells(crop_ref, g)
    for lo in range(0, STEP, 256):
        hi = min(lo + 256, STEP)
        reps = (hi - lo) // CH
        gain, bias = (jnp.concatenate([v_s[n]] * reps, axis=1) for n in range(2))
        hat, _ = hat_of(x[:, lo:hi])
        normed = (hat * gain + bias).astype(bf16)
        both = mm(w_s[...], normed, 1, 0)
        factor = (jnp.tanh(both[: 2 * CH]) + 1.0) * (both[2 * CH :] * live[:, lo:hi])
        f_ref[:, :, lo:hi] = factor.astype(bf16).reshape(PEERS, 2 * OWN, hi - lo)


def k1b(
    crop_ref, pair_ref, cot_ref, ig_ref, ib_ref, w_ref, gw_ref, n_ref, do_ref, e_ref, sv_ref, sg_ref,
    wg_s, wv_s, gw_s, v_s,
):
    g = pl.program_id(0)

    @pl.when(g == 0)
    def _():
        perm = interleave()
        gates, values = sides(w_ref[...])
        wg_s[...] = mm(perm, gates, 1, 1).astype(bf16)
        wv_s[...] = mm(perm, values, 1, 1).astype(bf16)
        gw_s[...] = gw_ref[...].astype(f32).T.astype(bf16)
        v_s[0] = column(ig_ref[...])
        v_s[1] = column(ib_ref[...])

    hat, _ = hat_of(turned(pair_ref))
    normed = (hat * wide(v_s[0]) + wide(v_s[1])).astype(bf16)
    n_ref[:CH, :] = normed
    n_ref[CH:, :] = jnp.ones((16, STEP), bf16)
    sig = sigmoid(mm(wg_s[...], normed, 1, 0))
    live_sig = sig * live_cells(crop_ref, g)
    sv_ref[...] = live_sig.astype(bf16)
    sg_ref[...] = (live_sig * mm(wv_s[...], normed, 1, 0) * (1.0 - sig)).astype(bf16)
    gate = sigmoid(mm(gw_s[...], normed, 1, 0))
    up = turned(cot_ref) * gate
    do_ref[...] = up.astype(bf16)
    e_ref[...] = up * (1.0 - gate)


def k2(y_ref, _, l_ref, r_ref, z_ref, x_s, p_s, l_s, r_s, sem):
    def spread(s, carry):
        r, c = peers_of(s)
        rows = y_ref[s].astype(f32)
        for g in range(STEPS):
            for k, v in enumerate(unfold(rows[:, g * STEP : (g + 1) * STEP])):
                x_s[r, pl.ds(c * WIDE + g * 8 + k, 2 * OWN, stride=PITCH), :] = v
        return carry

    lax.fori_loop(0, PEERS, spread, 0, unroll=8)
    lane = lax.broadcasted_iota(jnp.int32, (FULL, 128), 1)

    def matrix(t):
        parts = [jnp.where(lane < TALL, x_s[r, t * PITCH : t * PITCH + FULL, :], 0.0) for r in range(ROWS)]
        return jnp.concatenate(parts, axis=1)

    for h in range(OWN):
        left = matrix(h).astype(bf16)
        right = matrix(OWN + h).astype(bf16)
        l_s[h] = left
        r_s[h] = right
        product = mm(right, left, 0, 0)
        for r in range(ROWS):
            p_s[r, h * JPITCH : h * JPITCH + ROWS * 128, :] = product[:, r * 128 : (r + 1) * 128]

    copies = [pltpu.make_async_copy(l_s, l_ref, sem.at[0]), pltpu.make_async_copy(r_s, r_ref, sem.at[1])]
    for copy in copies:
        copy.start()

    def gather(s, carry):
        r, c = peers_of(s)
        first = (c >> 1) * 128 + (c & 1) * WIDE
        for g in range(STEPS):
            pieces = [p_s[r, pl.ds(first + g * 8 + k, OWN, stride=JPITCH), :] for k in range(8)]
            z_ref[s, :, g * STEP : (g + 1) * STEP] = fold(pieces).astype(bf16)
        return carry

    lax.fori_loop(0, PEERS, gather, 0, unroll=8)
    for copy in copies:
        copy.wait()


def k3(z_ref, do_ref, og_ref, ow_ref, dp_ref, z_s, b_s, sem):
    gain = wide(column(og_ref[...]))
    copies = []
    for g in range(STEPS):
        at = pl.ds(g * STEP, STEP)
        for d in range(PEERS):
            z_s[g, d * OWN : (d + 1) * OWN, :] = z_ref[d, :, at].astype(f32)
        hat, inverse = hat_of(z_s[g])
        scaled = mm(ow_ref[...], do_ref[:, at], 1, 0) * gain
        m1 = jnp.mean(scaled, axis=0, keepdims=True)
        m2 = jnp.mean(scaled * hat, axis=0, keepdims=True)
        z_s[g] = inverse * (scaled - m1 - hat * m2)
        for d in range(PEERS):
            b_s[d, :, at] = z_s[g, d * OWN : (d + 1) * OWN, :].astype(bf16)
        if copies:
            copies[-1].start()
        copies.append(pltpu.make_async_copy(b_s.at[:, :, at], dp_ref.at[:, :, at], sem.at[g]))
    copies[-1].start()
    for copy in copies:
        copy.wait()


def k3b(
    z_ref, n_ref, do_ref, e_ref, og_ref, ob_ref, ow_ref, dg_ref, gow_ref, gv_ref, gg_ref,
    z_s, owt_s, v_s,
):
    @pl.when(pl.program_id(0) == 0)
    def _():
        owt_s[...] = ow_ref[...].astype(f32).T.astype(bf16)
        v_s[0] = column(og_ref[...])
        v_s[1] = column(ob_ref[...])
        gow_ref[...] = jnp.zeros_like(gow_ref)
        gv_ref[...] = jnp.zeros_like(gv_ref)
        gg_ref[...] = jnp.zeros_like(gg_ref)

    for d in range(PEERS):
        z_s[d * OWN : (d + 1) * OWN, :] = z_ref[d].astype(f32)
    hat, _ = hat_of(z_s[...])
    tri = (hat * wide(v_s[0]) + wide(v_s[1])).astype(bf16)
    d_out = do_ref[...]
    d_gate = (e_ref[...] * mm(owt_s[...], tri, 1, 0)).astype(bf16)
    dg_ref[...] = d_gate
    gow_ref[...] += mm(tri, d_out, 1, 1)
    gg_ref[...] += mm(n_ref[...], d_gate, 1, 1)
    up = mm(ow_ref[...], d_out, 1, 0)
    gv_ref[0] += lane_fold(up * hat)
    gv_ref[1] += lane_fold(up)


def k4(dp_ref, l_ref, r_ref, _, a_ref, x_s, o_s, l_s, r_s, sem):
    copies = [pltpu.make_async_copy(l_ref, l_s, sem.at[0]), pltpu.make_async_copy(r_ref, r_s, sem.at[1])]
    for copy in copies:
        copy.start()
    zero = jnp.zeros((128 - TALL, 128), f32)
    for r in range(ROWS):
        for h in range(OWN):
            for q in range(ROWS):
                at = h * JPITCH + q * 128 + TALL
                x_s[r, at : at + 128 - TALL, :] = zero

    def spread(s, carry):
        r, c = peers_of(s)
        first = (c >> 1) * 128 + (c & 1) * WIDE
        rows = dp_ref[s].astype(f32)
        for g in range(STEPS):
            for k, v in enumerate(unfold(rows[:, g * STEP : (g + 1) * STEP])):
                x_s[r, pl.ds(first + g * 8 + k, OWN, stride=JPITCH), :] = v
        return carry

    lax.fori_loop(0, PEERS, spread, 0, unroll=16)
    for copy in copies:
        copy.wait()
    lane = lax.broadcasted_iota(jnp.int32, (ROWS * 128, 128), 1)
    for h in range(OWN):
        parts = []
        for r in range(ROWS):
            x = x_s[r, h * JPITCH : h * JPITCH + ROWS * 128, :]
            parts.append(jnp.where(lane < TALL, x, 0.0).astype(bf16))
        dp = jnp.concatenate(parts, axis=1)
        d_left = mm(r_s[h], dp, 1, 0)
        d_right = mm(l_s[h], dp, 1, 1)
        for r in range(ROWS):
            o_s[r, h * PITCH : h * PITCH + FULL, :] = d_left[:, r * 128 : (r + 1) * 128]
            at = (OWN + h) * PITCH
            o_s[r, at : at + FULL, :] = d_right[:, r * 128 : (r + 1) * 128]

    def gather(s, carry):
        r, c = peers_of(s)
        for g in range(STEPS):
            pieces = [o_s[r, pl.ds(c * WIDE + g * 8 + k, 2 * OWN, stride=PITCH), :] for k in range(8)]
            a_ref[s, :, g * STEP : (g + 1) * STEP] = fold(pieces).astype(bf16)
        return carry

    lax.fori_loop(0, PEERS, gather, 0, unroll=16)


def k5(
    a_ref, sv_ref, sg_ref, n_ref, ig_ref, ib_ref, w_ref, gw_ref, gow_ref, gv_ref, gg_ref,
    s_ref, ag_s, pk_s,
):
    total = None
    for g in range(STEPS):
        at = slice(g * STEP, (g + 1) * STEP)
        d = a_ref[:, :, at].reshape(2 * CH, STEP)
        slopes = jnp.concatenate([d * sg_ref[:, at], d * sv_ref[:, at]], axis=0)
        part = mm(slopes, n_ref[:, at], 1, 1)
        total = part if total is None else total + part
    ag_s[...] = total
    perm = interleave()
    gates, values = sides(w_ref[...])
    g_gates, g_values = ag_s[: 2 * CH, :].T, ag_s[2 * CH :, :].T
    weights = (mm(gates, perm, 1, 1), mm(values, perm, 1, 1), gw_ref[...].astype(f32))
    slope = jnp.zeros((CH, 1), f32)
    shift = jnp.zeros((CH, 1), f32)
    for weight, grad in zip(weights, (g_gates, g_values, gg_ref[...])):
        slope += jnp.sum(weight * grad[:CH, :], axis=1, keepdims=True)
        shift += jnp.sum(weight * grad[CH : CH + 1, :], axis=1, keepdims=True)
    gain, bias = column(ig_ref[...]), column(ib_ref[...])
    lane = lax.broadcasted_iota(jnp.int32, (CH, CH), 1)
    sums = jnp.where(lane == 0, (slope - bias * shift) / gain, jnp.where(lane == 1, shift, 0.0))
    for n in range(2):
        sums = jnp.where(lane == 2 + n, jnp.sum(gv_ref[n], axis=1, keepdims=True), sums)
    d_gates = mm(g_gates[:CH, :].astype(bf16), perm, 1, 0)
    d_values = mm(g_values[:CH, :].astype(bf16), perm, 1, 0)
    planes = (
        d_gates[:, :CH], d_values[:, :CH], d_gates[:, CH:], d_values[:, CH:],
        gg_ref[:CH, :], gow_ref[...], sums, jnp.zeros((CH, CH), f32),
    )
    for n, plane in enumerate(planes):
        pk_s[pl.ds(n, CH, stride=8), :] = plane
    s_ref[...] = pk_s[...].astype(bf16).reshape(CH, 8, CH)


def k5b(pair_ref, a_ref, sv_ref, sg_ref, dg_ref, ig_ref, w_ref, gw_ref, gp_ref, bk_s, v_s):
    @pl.when(pl.program_id(0) == 0)
    def _():
        perm = interleave()
        gates, values = sides(w_ref[...])
        bk_s[:, : 2 * CH] = mm(gates, perm, 1, 1).astype(bf16)
        bk_s[:, 2 * CH : 4 * CH] = mm(values, perm, 1, 1).astype(bf16)
        bk_s[:, 4 * CH :] = gw_ref[...]
        v_s[...] = column(ig_ref[...])

    hat, inverse = hat_of(turned(pair_ref))
    d = a_ref[...].reshape(2 * CH, STEP).astype(f32)
    d_gates = (d * sg_ref[...].astype(f32)).astype(bf16)
    d_values = (d * sv_ref[...].astype(f32)).astype(bf16)
    d_normed = mm(bk_s[...], jnp.concatenate([d_gates, d_values, dg_ref[...]], axis=0), 1, 0)
    scaled = d_normed * wide(v_s[...])
    m1 = jnp.mean(scaled, axis=0, keepdims=True)
    m2 = jnp.mean(scaled * hat, axis=0, keepdims=True)
    back = (inverse * (scaled - m1 - hat * m2)).T
    flat = gp_ref.reshape(STEP, CH)
    for k in range(8):
        flat[pl.ds(k, TALL, stride=8), :] = back[k * TALL : (k + 1) * TALL, :]


def k6(x_ref, _, o_ref):
    total = jnp.sum(x_ref[...].astype(f32), axis=0).astype(bf16)
    o_ref[...] = jnp.broadcast_to(total[None], o_ref.shape)


def k7(x_ref, gp_ref, gg_ref, gow_ref, *rest, factor):
    s_s = rest[-1]
    s_s[...] = x_ref[...].astype(f32).reshape(CH * 8, CH) * factor
    for q in range(4):
        gp_ref[:, q * CH : (q + 1) * CH] = s_s[pl.ds(q, CH, stride=8), :]
    gg_ref[...] = s_s[pl.ds(4, CH, stride=8), :]
    gow_ref[...] = s_s[pl.ds(5, CH, stride=8), :]
    sums = s_s[pl.ds(6, CH, stride=8), :].T
    for n in range(4):
        rest[n][...] = sums[n : n + 1]


def whole(*shape):
    return pl.BlockSpec(shape, lambda g: (0,) * len(shape))


def tile():
    return pl.BlockSpec((TALL, 8, CH), lambda g: (0, g, 0))


def lanes(*shape):
    return pl.BlockSpec((*shape, STEP), lambda g: (0,) * len(shape) + (g,))


SMEM = pl.BlockSpec(memory_space=pltpu.SMEM)
SMALL = pltpu.CompilerParams(vmem_limit_bytes=12 << 20)
LARGE = pltpu.CompilerParams(vmem_limit_bytes=22 << 20)
cost = pl.CostEstimate(flops=1_000_000_000, transcendentals=0, bytes_accessed=8_000_000)


def out(shape, dtype):
    return jax.ShapeDtypeStruct(shape, dtype)


def away(shape, dtype):
    return pltpu.HBM(shape, dtype)


def keep_away(*arrays):
    return [pltpu.with_memory_space_constraint(a, pltpu.HBM) for a in arrays]


def vm(*shape, dtype=f32):
    return pltpu.VMEM(shape, dtype)


HERE = pl.BlockSpec(memory_space=pltpu.VMEM)
AWAY = pl.BlockSpec(memory_space=pltpu.HBM)
KEPT = (OWN, FULL, ROWS * 128)


def product_call(factors, after, name):
    return pl.pallas_call(
        k2,
        name=name,
        compiler_params=LARGE,
        in_specs=[HERE, AWAY],
        out_specs=[AWAY, AWAY, HERE],
        out_shape=[away(KEPT, bf16), away(KEPT, bf16), out((PEERS, OWN, CELLS), bf16)],
        scratch_shapes=[
            vm(ROWS, 2 * OWN * PITCH, 128), vm(ROWS, OWN * JPITCH, 128),
            vm(*KEPT, dtype=bf16), vm(*KEPT, dtype=bf16), pltpu.SemaphoreType.DMA((2,)),
        ],
    )(factors, *keep_away(after))


def slopes_call(d_product, left, right, after, name):
    return pl.pallas_call(
        k4,
        name=name,
        compiler_params=LARGE,
        in_specs=[HERE, AWAY, AWAY, AWAY],
        out_specs=HERE,
        out_shape=out((PEERS, 2 * OWN, CELLS), bf16),
        scratch_shapes=[
            vm(ROWS, OWN * JPITCH, 128), vm(ROWS, 2 * OWN * PITCH, 128),
            vm(*KEPT, dtype=bf16), vm(*KEPT, dtype=bf16), pltpu.SemaphoreType.DMA((2,)),
        ],
    )(d_product, *keep_away(left, right, after))


def per_device(
    pair,
    cotangent,
    crop_length,
    in_gain,
    in_bias,
    proj_weight,
    gate_weight,
    out_gain,
    out_bias,
    out_weight,
):
    group = ("row", "col")
    everyone = ("samp", "row", "col")
    swap = functools.partial(lax.all_to_all, split_axis=0, concat_axis=0, tiled=True)
    row = lambda v: v.reshape(1, CH)
    wb = functools.partial(vm, dtype=bf16)
    pair, cotangent = pair[0], cotangent[0]
    in_gain, in_bias, out_gain, out_bias = map(row, (in_gain, in_bias, out_gain, out_bias))
    one, square, proj = whole(1, CH), whole(CH, CH), whole(CH, 4 * CH)
    both = (PEERS, 2 * OWN, CELLS)
    factors = pl.pallas_call(
        k1,
        name="factors",
        compiler_params=SMALL,
        grid=(STEPS,),
        in_specs=[SMEM, tile(), one, one, proj],
        out_specs=lanes(PEERS, 2 * OWN),
        out_shape=out(both, bf16),
        scratch_shapes=[wb(4 * CH, CH), vm(2, CH, CH)],
    )(crop_length, *keep_away(pair, in_gain, in_bias, proj_weight))
    factors = swap(factors, group)
    normed, d_out, slope, by_value, by_gate = pl.pallas_call(
        k1b,
        name="gate",
        compiler_params=SMALL,
        grid=(STEPS,),
        in_specs=[SMEM, tile(), tile(), one, one, proj, square],
        out_specs=[lanes(CH + 16), lanes(CH), lanes(CH), lanes(2 * CH), lanes(2 * CH)],
        out_shape=[
            away((CH + 16, CELLS), bf16), away((CH, CELLS), bf16), away((CH, CELLS), f32),
            away((2 * CH, CELLS), bf16), away((2 * CH, CELLS), bf16),
        ],
        scratch_shapes=[wb(2 * CH, CH), wb(2 * CH, CH), wb(CH, CH), vm(2, CH, CH)],
        cost_estimate=cost,
    )(crop_length, *keep_away(pair, cotangent, in_gain, in_bias, proj_weight, gate_weight))
    left, right, product = product_call(factors, d_out, "product")
    product = swap(product, group)
    d_product = pl.pallas_call(
        k3,
        name="middle",
        compiler_params=SMALL,
        in_specs=[HERE] * 4,
        out_specs=AWAY,
        out_shape=away((PEERS, OWN, CELLS), bf16),
        scratch_shapes=[vm(STEPS, CH, STEP), wb(PEERS, OWN, CELLS), pltpu.SemaphoreType.DMA((STEPS,))],
    )(product, d_out, out_gain, out_weight)
    d_product = swap(d_product, group)
    d_gate, g_out_weight, g_out, g_gate = pl.pallas_call(
        k3b,
        name="outputs",
        compiler_params=SMALL,
        grid=(STEPS,),
        in_specs=[lanes(PEERS, OWN), lanes(CH + 16), lanes(CH), lanes(CH), one, one, square],
        out_specs=[lanes(CH), square, whole(2, CH, CH), whole(CH + 16, CH)],
        out_shape=[
            away((CH, CELLS), bf16), away((CH, CH), f32), away((2, CH, CH), f32), away((CH + 16, CH), f32),
        ],
        scratch_shapes=[vm(CH, STEP), wb(CH, CH), vm(2, CH, CH)],
        cost_estimate=cost,
    )(product, *keep_away(normed, d_out, slope, out_gain, out_bias, out_weight))
    d_factors = slopes_call(d_product, left, right, d_gate, "slopes")
    d_factors = swap(d_factors, group)
    packed = pl.pallas_call(
        k5,
        name="weights",
        compiler_params=SMALL,
        in_specs=[HERE] * 11,
        out_specs=HERE,
        out_shape=out((CH, 8, CH), bf16),
        scratch_shapes=[vm(4 * CH, CH + 16), vm(CH * 8, CH)],
    )(d_factors, by_value, by_gate, normed, in_gain, in_bias, proj_weight, gate_weight,
      g_out_weight, g_out, g_gate)
    parts = swap(packed, everyone)
    grad_pair = pl.pallas_call(
        k5b,
        name="inputs",
        compiler_params=SMALL,
        grid=(STEPS,),
        in_specs=[
            tile(), lanes(PEERS, 2 * OWN), lanes(2 * CH), lanes(2 * CH), lanes(CH), one, proj, square,
        ],
        out_specs=tile(),
        out_shape=out((TALL, WIDE, CH), f32),
        scratch_shapes=[wb(CH, 5 * CH), vm(CH, CH)],
        cost_estimate=cost,
    )(*keep_away(pair), d_factors, *keep_away(by_value, by_gate, d_gate, in_gain, proj_weight, gate_weight))
    total = pl.pallas_call(
        k6,
        name="total",
        compiler_params=SMALL,
        in_specs=[HERE, AWAY],
        out_specs=HERE,
        out_shape=out((CH, 8, CH), bf16),
    )(parts, *keep_away(grad_pair))
    total = swap(total, everyone)
    g_proj_weight, g_gate_weight, g_out_weight, *sums = pl.pallas_call(
        functools.partial(k7, factor=1.0 / FULL),
        name="unpack",
        compiler_params=SMALL,
        out_shape=[out((CH, 4 * CH), f32), out((CH, CH), f32), out((CH, CH), f32)] + [out((1, CH), f32)] * 4,
        scratch_shapes=[vm(CH * 8, CH)],
    )(total)
    sums = [s.reshape(CH) for s in sums]
    return (
        grad_pair[None],
        sums[0],
        sums[1],
        g_proj_weight,
        g_gate_weight,
        sums[2],
        sums[3],
        g_out_weight,
    )


def solution(mesh):
    return jax.shard_map(
        per_device,
        mesh=mesh,
        in_specs=(
            P("samp", "row", "col", None),
            P("samp", "row", "col", None),
            P("samp"),
            P(),
            P(),
            P(),
            P(),
            P(),
            P(),
            P(),
        ),
        out_specs=(P("samp", "row", "col", None), P(), P(), P(), P(), P(), P(), P()),
        check_vma=False,
    )
```

```python
import functools

import jax
import jax.numpy as jnp
from jax import lax
from jax.experimental import pallas as pl
from jax.experimental.pallas import tpu as pltpu
from jax.sharding import PartitionSpec as P

epsilon = 1e-05

TALL = 80
WIDE = 40
CH = 128
ROWS = 4
COLS = 8
PEERS = ROWS * COLS
OWN = CH // PEERS
CELLS = TALL * WIDE
STEP = 8 * TALL
STEPS = CELLS // STEP
FULL = COLS * WIDE
PITCH = FULL + 8
JPITCH = ROWS * 128 + 8
f32 = jnp.float32
bf16 = jnp.bfloat16


def mm(a, b, ca, cb):
    return lax.dot_general(a, b, (((ca,), (cb,)), ((), ())), preferred_element_type=f32)


def sigmoid(x):
    return 0.5 * jnp.tanh(0.5 * x) + 0.5


def column(row):
    return jnp.broadcast_to(row, (CH, CH)).T


def wide(col):
    return jnp.concatenate([col] * (STEP // CH), axis=1)


def interleave():
    n = 2 * CH
    q = lax.broadcasted_iota(jnp.int32, (n, n), 0)
    p = lax.broadcasted_iota(jnp.int32, (n, n), 1)
    src = ((q >> 2) & 1) * CH + (q >> 3) * OWN + (q & 3)
    return jnp.where(src == p, 1.0, 0.0).astype(bf16)


def turned(ref):
    flat = ref.reshape(STEP, CH)
    rows = [flat[pl.ds(k, TALL, stride=8), :] for k in range(8)]
    return jnp.concatenate(rows, axis=0).T


def live_cells(crop_ref, g):
    lane = lax.broadcasted_iota(jnp.int32, (1, STEP), 1)
    k = jnp.zeros((1, STEP), jnp.int32)
    for m in range(1, 8):
        k = k + jnp.where(lane >= m * TALL, 1, 0)
    i = lane - k * TALL + lax.axis_index("row") * TALL
    k = k + (g * 8 + lax.axis_index("col") * WIDE)
    live = jnp.logical_and(i < crop_ref[0], k < crop_ref[0])
    return jnp.where(live, 1.0, 0.0).astype(f32)


def hat_of(x):
    centre = jnp.mean(x, axis=0, keepdims=True)
    centered = x - centre
    inverse = lax.rsqrt(jnp.mean(centered * centered, axis=0, keepdims=True) + epsilon)
    return centered * inverse, inverse


def lane_fold(x):
    out = x[:, :CH]
    for m in range(1, x.shape[1] // CH):
        out = out + x[:, m * CH : (m + 1) * CH]
    return out


def peers_of(s):
    return s >> 3, s & 7


def unfold(rows):
    n = rows.shape[0]
    lane = lax.broadcasted_iota(jnp.int32, (n, 128), 1)
    out = []
    for k in range(8):
        at = k * TALL
        m, off = at // 128, at % 128
        v = rows[:, m * 128 : (m + 1) * 128]
        if off + TALL > 128:
            v = jnp.where(lane >= off, v, rows[:, (m + 1) * 128 : (m + 2) * 128])
        out.append(pltpu.roll(v, 128 - off, 1) if off else v)
    return out


def fold(pieces):
    n = pieces[0].shape[0]
    lane = lax.broadcasted_iota(jnp.int32, (n, 128), 1)
    r = [pltpu.roll(p, (k * TALL) % 128, 1) if k else p for k, p in enumerate(pieces)]
    cols = []
    for m in range(STEP // 128):
        lo, hi = m * 128, (m + 1) * 128
        v = None
        for k in range(8):
            a, b = max(lo, k * TALL), min(hi, (k + 1) * TALL)
            if a >= b:
                continue
            v = r[k] if v is None else jnp.where(lane >= a - lo, r[k], v)
        cols.append(v)
    return jnp.concatenate(cols, axis=1)


def sides(w):
    gates = jnp.concatenate([w[:, :CH], w[:, 2 * CH : 3 * CH]], axis=1)
    values = jnp.concatenate([w[:, CH : 2 * CH], w[:, 3 * CH :]], axis=1)
    return gates, values


def k1(crop_ref, pair_ref, ig_ref, ib_ref, w_ref, f_ref, w_s, v_s):
    g = pl.program_id(0)

    @pl.when(g == 0)
    def _():
        perm = interleave()
        gates, values = sides(w_ref[...])
        w_s[: 2 * CH, :] = (0.5 * mm(perm, gates, 1, 1)).astype(bf16)
        w_s[2 * CH :, :] = (0.5 * mm(perm, values, 1, 1)).astype(bf16)
        v_s[0] = column(ig_ref[...])
        v_s[1] = column(ib_ref[...])

    x = turned(pair_ref)
    live = live_cells(crop_ref, g)
    for lo in range(0, STEP, 256):
        hi = min(lo + 256, STEP)
        reps = (hi - lo) // CH
        gain, bias = (jnp.concatenate([v_s[n]] * reps, axis=1) for n in range(2))
        hat, _ = hat_of(x[:, lo:hi])
        normed = (hat * gain + bias).astype(bf16)
        both = mm(w_s[...], normed, 1, 0)
        factor = (jnp.tanh(both[: 2 * CH]) + 1.0) * (both[2 * CH :] * live[:, lo:hi])
        f_ref[:, :, lo:hi] = factor.astype(bf16).reshape(PEERS, 2 * OWN, hi - lo)


def k1b(
    crop_ref, pair_ref, cot_ref, ig_ref, ib_ref, w_ref, gw_ref, n_ref, do_ref, e_ref, sv_ref, sg_ref,
    wg_s, wv_s, gw_s, v_s,
):
    g = pl.program_id(0)

    @pl.when(g == 0)
    def _():
        perm = interleave()
        gates, values = sides(w_ref[...])
        wg_s[...] = mm(perm, gates, 1, 1).astype(bf16)
        wv_s[...] = mm(perm, values, 1, 1).astype(bf16)
        gw_s[...] = gw_ref[...].astype(f32).T.astype(bf16)
        v_s[0] = column(ig_ref[...])
        v_s[1] = column(ib_ref[...])

    hat, _ = hat_of(turned(pair_ref))
    normed = (hat * wide(v_s[0]) + wide(v_s[1])).astype(bf16)
    n_ref[:CH, :] = normed
    n_ref[CH:, :] = jnp.ones((16, STEP), bf16)
    sig = sigmoid(mm(wg_s[...], normed, 1, 0))
    live_sig = sig * live_cells(crop_ref, g)
    sv_ref[...] = live_sig.astype(bf16)
    sg_ref[...] = (live_sig * mm(wv_s[...], normed, 1, 0) * (1.0 - sig)).astype(bf16)
    gate = sigmoid(mm(gw_s[...], normed, 1, 0))
    up = turned(cot_ref) * gate
    do_ref[...] = up.astype(bf16)
    e_ref[...] = up * (1.0 - gate)


def k2(y_ref, _, l_ref, r_ref, z_ref, x_s, p_s, l_s, r_s, sem):
    def spread(s, carry):
        r, c = peers_of(s)
        rows = y_ref[s].astype(f32)
        for g in range(STEPS):
            for k, v in enumerate(unfold(rows[:, g * STEP : (g + 1) * STEP])):
                x_s[r, pl.ds(c * WIDE + g * 8 + k, 2 * OWN, stride=PITCH), :] = v
        return carry

    lax.fori_loop(0, PEERS, spread, 0, unroll=16)
    lane = lax.broadcasted_iota(jnp.int32, (FULL, 128), 1)

    def matrix(t):
        parts = [jnp.where(lane < TALL, x_s[r, t * PITCH : t * PITCH + FULL, :], 0.0) for r in range(ROWS)]
        return jnp.concatenate(parts, axis=1)

    for h in range(OWN):
        left = matrix(h).astype(bf16)
        right = matrix(OWN + h).astype(bf16)
        l_s[h] = left
        r_s[h] = right
        product = mm(right, left, 0, 0)
        for r in range(ROWS):
            p_s[r, h * JPITCH : h * JPITCH + ROWS * 128, :] = product[:, r * 128 : (r + 1) * 128]

    copies = [pltpu.make_async_copy(l_s, l_ref, sem.at[0]), pltpu.make_async_copy(r_s, r_ref, sem.at[1])]
    for copy in copies:
        copy.start()

    def gather(s, carry):
        r, c = peers_of(s)
        first = (c >> 1) * 128 + (c & 1) * WIDE
        for g in range(STEPS):
            pieces = [p_s[r, pl.ds(first + g * 8 + k, OWN, stride=JPITCH), :] for k in range(8)]
            z_ref[s, :, g * STEP : (g + 1) * STEP] = fold(pieces).astype(bf16)
        return carry

    lax.fori_loop(0, PEERS, gather, 0, unroll=16)
    for copy in copies:
        copy.wait()


def k3(z_ref, do_ref, og_ref, ow_ref, dp_ref, z_s, b_s, sem):
    gain = wide(column(og_ref[...]))
    copies = []
    for g in range(STEPS):
        at = pl.ds(g * STEP, STEP)
        for d in range(PEERS):
            z_s[g, d * OWN : (d + 1) * OWN, :] = z_ref[d, :, at].astype(f32)
        hat, inverse = hat_of(z_s[g])
        scaled = mm(ow_ref[...], do_ref[:, at], 1, 0) * gain
        m1 = jnp.mean(scaled, axis=0, keepdims=True)
        m2 = jnp.mean(scaled * hat, axis=0, keepdims=True)
        z_s[g] = inverse * (scaled - m1 - hat * m2)
        for d in range(PEERS):
            b_s[d, :, at] = z_s[g, d * OWN : (d + 1) * OWN, :].astype(bf16)
        if copies:
            copies[-1].start()
        copies.append(pltpu.make_async_copy(b_s.at[:, :, at], dp_ref.at[:, :, at], sem.at[g]))
    copies[-1].start()
    for copy in copies:
        copy.wait()


def k3b(
    z_ref, n_ref, do_ref, e_ref, og_ref, ob_ref, ow_ref, dg_ref, gow_ref, gv_ref, gg_ref,
    z_s, owt_s, v_s,
):
    @pl.when(pl.program_id(0) == 0)
    def _():
        owt_s[...] = ow_ref[...].astype(f32).T.astype(bf16)
        v_s[0] = column(og_ref[...])
        v_s[1] = column(ob_ref[...])
        gow_ref[...] = jnp.zeros_like(gow_ref)
        gv_ref[...] = jnp.zeros_like(gv_ref)
        gg_ref[...] = jnp.zeros_like(gg_ref)

    for d in range(PEERS):
        z_s[d * OWN : (d + 1) * OWN, :] = z_ref[d].astype(f32)
    hat, _ = hat_of(z_s[...])
    tri = (hat * wide(v_s[0]) + wide(v_s[1])).astype(bf16)
    d_out = do_ref[...]
    d_gate = (e_ref[...] * mm(owt_s[...], tri, 1, 0)).astype(bf16)
    dg_ref[...] = d_gate
    gow_ref[...] += mm(tri, d_out, 1, 1)
    gg_ref[...] += mm(n_ref[...], d_gate, 1, 1)
    up = mm(ow_ref[...], d_out, 1, 0)
    gv_ref[0] += lane_fold(up * hat)
    gv_ref[1] += lane_fold(up)


def k4(dp_ref, l_ref, r_ref, _, a_ref, x_s, o_s, l_s, r_s, sem):
    copies = [pltpu.make_async_copy(l_ref, l_s, sem.at[0]), pltpu.make_async_copy(r_ref, r_s, sem.at[1])]
    for copy in copies:
        copy.start()
    zero = jnp.zeros((128 - TALL, 128), f32)
    for r in range(ROWS):
        for h in range(OWN):
            for q in range(ROWS):
                at = h * JPITCH + q * 128 + TALL
                x_s[r, at : at + 128 - TALL, :] = zero

    def spread(s, carry):
        r, c = peers_of(s)
        first = (c >> 1) * 128 + (c & 1) * WIDE
        rows = dp_ref[s].astype(f32)
        for g in range(STEPS):
            for k, v in enumerate(unfold(rows[:, g * STEP : (g + 1) * STEP])):
                x_s[r, pl.ds(first + g * 8 + k, OWN, stride=JPITCH), :] = v
        return carry

    lax.fori_loop(0, PEERS, spread, 0, unroll=16)
    for copy in copies:
        copy.wait()
    lane = lax.broadcasted_iota(jnp.int32, (ROWS * 128, 128), 1)
    for h in range(OWN):
        parts = []
        for r in range(ROWS):
            x = x_s[r, h * JPITCH : h * JPITCH + ROWS * 128, :]
            parts.append(jnp.where(lane < TALL, x, 0.0).astype(bf16))
        dp = jnp.concatenate(parts, axis=1)
        d_left = mm(r_s[h], dp, 1, 0)
        d_right = mm(l_s[h], dp, 1, 1)
        for r in range(ROWS):
            o_s[r, h * PITCH : h * PITCH + FULL, :] = d_left[:, r * 128 : (r + 1) * 128]
            at = (OWN + h) * PITCH
            o_s[r, at : at + FULL, :] = d_right[:, r * 128 : (r + 1) * 128]

    def gather(s, carry):
        r, c = peers_of(s)
        for g in range(STEPS):
            pieces = [o_s[r, pl.ds(c * WIDE + g * 8 + k, 2 * OWN, stride=PITCH), :] for k in range(8)]
            a_ref[s, :, g * STEP : (g + 1) * STEP] = fold(pieces).astype(bf16)
        return carry

    lax.fori_loop(0, PEERS, gather, 0, unroll=16)


def k5(
    a_ref, sv_ref, sg_ref, n_ref, ig_ref, ib_ref, w_ref, gw_ref, gow_ref, gv_ref, gg_ref,
    s_ref, ag_s, pk_s,
):
    total = None
    for g in range(STEPS):
        at = slice(g * STEP, (g + 1) * STEP)
        d = a_ref[:, :, at].reshape(2 * CH, STEP)
        slopes = jnp.concatenate([d * sg_ref[:, at], d * sv_ref[:, at]], axis=0)
        part = mm(slopes, n_ref[:, at], 1, 1)
        total = part if total is None else total + part
    ag_s[...] = total
    perm = interleave()
    gates, values = sides(w_ref[...])
    g_gates, g_values = ag_s[: 2 * CH, :].T, ag_s[2 * CH :, :].T
    weights = (mm(gates, perm, 1, 1), mm(values, perm, 1, 1), gw_ref[...].astype(f32))
    slope = jnp.zeros((CH, 1), f32)
    shift = jnp.zeros((CH, 1), f32)
    for weight, grad in zip(weights, (g_gates, g_values, gg_ref[...])):
        slope += jnp.sum(weight * grad[:CH, :], axis=1, keepdims=True)
        shift += jnp.sum(weight * grad[CH : CH + 1, :], axis=1, keepdims=True)
    gain, bias = column(ig_ref[...]), column(ib_ref[...])
    lane = lax.broadcasted_iota(jnp.int32, (CH, CH), 1)
    sums = jnp.where(lane == 0, (slope - bias * shift) / gain, jnp.where(lane == 1, shift, 0.0))
    for n in range(2):
        sums = jnp.where(lane == 2 + n, jnp.sum(gv_ref[n], axis=1, keepdims=True), sums)
    d_gates = mm(g_gates[:CH, :].astype(bf16), perm, 1, 0)
    d_values = mm(g_values[:CH, :].astype(bf16), perm, 1, 0)
    planes = (
        d_gates[:, :CH], d_values[:, :CH], d_gates[:, CH:], d_values[:, CH:],
        gg_ref[:CH, :], gow_ref[...], sums, jnp.zeros((CH, CH), f32),
    )
    for n, plane in enumerate(planes):
        pk_s[pl.ds(n, CH, stride=8), :] = plane
    s_ref[...] = pk_s[...].astype(bf16).reshape(CH, 8, CH)


def k5b(pair_ref, a_ref, sv_ref, sg_ref, dg_ref, ig_ref, w_ref, gw_ref, gp_ref, bk_s, v_s):
    @pl.when(pl.program_id(0) == 0)
    def _():
        perm = interleave()
        gates, values = sides(w_ref[...])
        bk_s[:, : 2 * CH] = mm(gates, perm, 1, 1).astype(bf16)
        bk_s[:, 2 * CH : 4 * CH] = mm(values, perm, 1, 1).astype(bf16)
        bk_s[:, 4 * CH :] = gw_ref[...]
        v_s[...] = column(ig_ref[...])

    hat, inverse = hat_of(turned(pair_ref))
    d = a_ref[...].reshape(2 * CH, STEP).astype(f32)
    d_gates = (d * sg_ref[...].astype(f32)).astype(bf16)
    d_values = (d * sv_ref[...].astype(f32)).astype(bf16)
    d_normed = mm(bk_s[...], jnp.concatenate([d_gates, d_values, dg_ref[...]], axis=0), 1, 0)
    scaled = d_normed * wide(v_s[...])
    m1 = jnp.mean(scaled, axis=0, keepdims=True)
    m2 = jnp.mean(scaled * hat, axis=0, keepdims=True)
    back = (inverse * (scaled - m1 - hat * m2)).T
    flat = gp_ref.reshape(STEP, CH)
    for k in range(8):
        flat[pl.ds(k, TALL, stride=8), :] = back[k * TALL : (k + 1) * TALL, :]


def k6(x_ref, o_ref):
    total = jnp.sum(x_ref[...].astype(f32), axis=0).astype(bf16)
    o_ref[...] = jnp.broadcast_to(total[None], o_ref.shape)


def k7(x_ref, gp_ref, gg_ref, gow_ref, *rest, factor):
    s_s = rest[-1]
    s_s[...] = x_ref[...].astype(f32).reshape(CH * 8, CH) * factor
    for q in range(4):
        gp_ref[:, q * CH : (q + 1) * CH] = s_s[pl.ds(q, CH, stride=8), :]
    gg_ref[...] = s_s[pl.ds(4, CH, stride=8), :]
    gow_ref[...] = s_s[pl.ds(5, CH, stride=8), :]
    sums = s_s[pl.ds(6, CH, stride=8), :].T
    for n in range(4):
        rest[n][...] = sums[n : n + 1]


def whole(*shape):
    return pl.BlockSpec(shape, lambda g: (0,) * len(shape))


def tile():
    return pl.BlockSpec((TALL, 8, CH), lambda g: (0, g, 0))


def lanes(*shape):
    return pl.BlockSpec((*shape, STEP), lambda g: (0,) * len(shape) + (g,))


SMEM = pl.BlockSpec(memory_space=pltpu.SMEM)
SMALL = pltpu.CompilerParams(vmem_limit_bytes=12 << 20)
LARGE = pltpu.CompilerParams(vmem_limit_bytes=22 << 20)
cost = pl.CostEstimate(flops=1_000_000_000, transcendentals=0, bytes_accessed=8_000_000)


def out(shape, dtype):
    return jax.ShapeDtypeStruct(shape, dtype)


def away(shape, dtype):
    return pltpu.HBM(shape, dtype)


def keep_away(*arrays):
    return [pltpu.with_memory_space_constraint(a, pltpu.HBM) for a in arrays]


def vm(*shape, dtype=f32):
    return pltpu.VMEM(shape, dtype)


HERE = pl.BlockSpec(memory_space=pltpu.VMEM)
AWAY = pl.BlockSpec(memory_space=pltpu.HBM)
KEPT = (OWN, FULL, ROWS * 128)


def product_call(factors, after, name):
    return pl.pallas_call(
        k2,
        name=name,
        compiler_params=LARGE,
        in_specs=[HERE, AWAY],
        out_specs=[AWAY, AWAY, HERE],
        out_shape=[away(KEPT, bf16), away(KEPT, bf16), out((PEERS, OWN, CELLS), bf16)],
        scratch_shapes=[
            vm(ROWS, 2 * OWN * PITCH, 128), vm(ROWS, OWN * JPITCH, 128),
            vm(*KEPT, dtype=bf16), vm(*KEPT, dtype=bf16), pltpu.SemaphoreType.DMA((2,)),
        ],
    )(factors, *keep_away(after))


def slopes_call(d_product, left, right, after, name):
    return pl.pallas_call(
        k4,
        name=name,
        compiler_params=LARGE,
        in_specs=[HERE, AWAY, AWAY, AWAY],
        out_specs=HERE,
        out_shape=out((PEERS, 2 * OWN, CELLS), bf16),
        scratch_shapes=[
            vm(ROWS, OWN * JPITCH, 128), vm(ROWS, 2 * OWN * PITCH, 128),
            vm(*KEPT, dtype=bf16), vm(*KEPT, dtype=bf16), pltpu.SemaphoreType.DMA((2,)),
        ],
    )(d_product, *keep_away(left, right, after))


def per_device(
    pair,
    cotangent,
    crop_length,
    in_gain,
    in_bias,
    proj_weight,
    gate_weight,
    out_gain,
    out_bias,
    out_weight,
):
    group = ("row", "col")
    everyone = ("samp", "row", "col")
    swap = functools.partial(lax.all_to_all, split_axis=0, concat_axis=0, tiled=True)
    row = lambda v: v.reshape(1, CH)
    wb = functools.partial(vm, dtype=bf16)
    pair, cotangent = pair[0], cotangent[0]
    in_gain, in_bias, out_gain, out_bias = map(row, (in_gain, in_bias, out_gain, out_bias))
    one, square, proj = whole(1, CH), whole(CH, CH), whole(CH, 4 * CH)
    both = (PEERS, 2 * OWN, CELLS)
    factors = pl.pallas_call(
        k1,
        name="factors",
        compiler_params=SMALL,
        grid=(STEPS,),
        in_specs=[SMEM, tile(), one, one, proj],
        out_specs=lanes(PEERS, 2 * OWN),
        out_shape=out(both, bf16),
        scratch_shapes=[wb(4 * CH, CH), vm(2, CH, CH)],
    )(crop_length, *keep_away(pair, in_gain, in_bias, proj_weight))
    factors = swap(factors, group)
    normed, d_out, slope, by_value, by_gate = pl.pallas_call(
        k1b,
        name="gate",
        compiler_params=SMALL,
        grid=(STEPS,),
        in_specs=[SMEM, tile(), tile(), one, one, proj, square],
        out_specs=[lanes(CH + 16), lanes(CH), lanes(CH), lanes(2 * CH), lanes(2 * CH)],
        out_shape=[
            away((CH + 16, CELLS), bf16), away((CH, CELLS), bf16), away((CH, CELLS), f32),
            away((2 * CH, CELLS), bf16), away((2 * CH, CELLS), bf16),
        ],
        scratch_shapes=[wb(2 * CH, CH), wb(2 * CH, CH), wb(CH, CH), vm(2, CH, CH)],
        cost_estimate=cost,
    )(crop_length, *keep_away(pair, cotangent, in_gain, in_bias, proj_weight, gate_weight))
    left, right, product = product_call(factors, d_out, "product")
    product = swap(product, group)
    d_product = pl.pallas_call(
        k3,
        name="middle",
        compiler_params=SMALL,
        in_specs=[HERE] * 4,
        out_specs=AWAY,
        out_shape=away((PEERS, OWN, CELLS), bf16),
        scratch_shapes=[vm(STEPS, CH, STEP), wb(PEERS, OWN, CELLS), pltpu.SemaphoreType.DMA((STEPS,))],
    )(product, d_out, out_gain, out_weight)
    d_product = swap(d_product, group)
    d_gate, g_out_weight, g_out, g_gate = pl.pallas_call(
        k3b,
        name="outputs",
        compiler_params=SMALL,
        grid=(STEPS,),
        in_specs=[lanes(PEERS, OWN), lanes(CH + 16), lanes(CH), lanes(CH), one, one, square],
        out_specs=[lanes(CH), square, whole(2, CH, CH), whole(CH + 16, CH)],
        out_shape=[
            away((CH, CELLS), bf16), away((CH, CH), f32), away((2, CH, CH), f32), away((CH + 16, CH), f32),
        ],
        scratch_shapes=[vm(CH, STEP), wb(CH, CH), vm(2, CH, CH)],
        cost_estimate=cost,
    )(product, *keep_away(normed, d_out, slope, out_gain, out_bias, out_weight))
    d_factors = slopes_call(d_product, left, right, d_gate, "slopes")
    d_factors = swap(d_factors, group)
    packed = pl.pallas_call(
        k5,
        name="weights",
        compiler_params=SMALL,
        in_specs=[HERE] * 11,
        out_specs=HERE,
        out_shape=out((CH, 8, CH), bf16),
        scratch_shapes=[vm(4 * CH, CH + 16), vm(CH * 8, CH)],
    )(d_factors, by_value, by_gate, normed, in_gain, in_bias, proj_weight, gate_weight,
      g_out_weight, g_out, g_gate)
    parts = swap(packed, everyone)
    grad_pair = pl.pallas_call(
        k5b,
        name="inputs",
        compiler_params=SMALL,
        grid=(STEPS,),
        in_specs=[
            tile(), lanes(PEERS, 2 * OWN), lanes(2 * CH), lanes(2 * CH), lanes(CH), one, proj, square,
        ],
        out_specs=tile(),
        out_shape=out((TALL, WIDE, CH), f32),
        scratch_shapes=[wb(CH, 5 * CH), vm(CH, CH)],
        cost_estimate=cost,
    )(*keep_away(pair), d_factors, *keep_away(by_value, by_gate, d_gate, in_gain, proj_weight, gate_weight))
    total = pl.pallas_call(k6, name="total", compiler_params=SMALL, out_shape=out((CH, 8, CH), bf16))(parts)
    total = swap(total, everyone)
    g_proj_weight, g_gate_weight, g_out_weight, *sums = pl.pallas_call(
        functools.partial(k7, factor=1.0 / FULL),
        name="unpack",
        compiler_params=SMALL,
        out_shape=[out((CH, 4 * CH), f32), out((CH, CH), f32), out((CH, CH), f32)] + [out((1, CH), f32)] * 4,
        scratch_shapes=[vm(CH * 8, CH)],
    )(total)
    sums = [s.reshape(CH) for s in sums]
    return (
        grad_pair[None],
        sums[0],
        sums[1],
        g_proj_weight,
        g_gate_weight,
        sums[2],
        sums[3],
        g_out_weight,
    )


def solution(mesh):
    return jax.shard_map(
        per_device,
        mesh=mesh,
        in_specs=(
            P("samp", "row", "col", None),
            P("samp", "row", "col", None),
            P("samp"),
            P(),
            P(),
            P(),
            P(),
            P(),
            P(),
            P(),
        ),
        out_specs=(P("samp", "row", "col", None), P(), P(), P(), P(), P(), P(), P()),
        check_vma=False,
    )
```
